32 devices in a mesh: grp: 4 (over z), slab: 8 (over y, x, core).
Axes of the slice: x: 2, y: 2, z: 4, core: 2. Of those that a mesh axis runs over, the one named last changes fastest.
Arguments:
- tensor: float32 [672, 64, 672], P('grp', 'slab'), may hold values from -20 to 20
- start_one: float32 [672, 96], replicated, may hold values from -6 to 6
- start_two: float32 [672, 96], replicated, may hold values from -6 to 6
Outputs:
- basis_one: float32 [672, 96], replicated
- basis_two: float32 [672, 96], replicated
- core: float32 [96, 64, 96], P('grp', 'slab')
The draws below stay inside these ranges and needn't reach their ends.
All inputs are finite; a program needn't handle non-finite values.
Results may differ from the reference program's by a relative error of at most 0.0003.
Values sent between devices are 32-bit elements; how exact they have to be, the bound alone decides.
No kernel may reach another device: no remote copies, remote signals or barrier semaphores. Data moves between devices by JAX's collectives and lax.ppermute only.
A program may use at most 64 MiB of HBM per device.

```python
import jax
import jax.numpy as jnp
from jax import lax

N1 = 672
N2 = 672
RANK1 = 96
RANK2 = 96
ITERS = 2
COLS = 64


def draw_tensor(key, part):
    modes = 2 * RANK1 + RANK1 // 2
    key_power = jax.random.fold_in(key, 11)
    key_second = jax.random.fold_in(key, 23)
    key_columns = jax.random.fold_in(key, 37)
    key_first = jax.random.fold_in(key, 41)
    key_noise = jax.random.fold_in(key, 53)
    key_colscale = jax.random.fold_in(key, 67)
    key_rowscale = jax.random.fold_in(key, 79)
    index = jnp.arange(modes, dtype=jnp.float32)
    strong = index < RANK1
    top_pos = index / max(RANK1 - 1, 1)
    tail_pos = (index - RANK1) / max(modes - RANK1 - 1, 1)
    level = jnp.where(strong, top_pos * jnp.log(0.3), jnp.log(0.1) + tail_pos * jnp.log(0.3))
    jitter = jax.random.uniform(key_power, (modes,), jnp.float32, jnp.log(0.8), jnp.log(1.25))
    power = jnp.exp(level + jitter)
    amplitude = jnp.sqrt(power / jnp.sum(power))
    second = jax.random.normal(key_second, (N2, modes), jnp.float32)
    columns = jax.random.normal(key_columns, (COLS, modes), jnp.float32)
    first = jax.random.normal(key_first, (N1, modes), jnp.float32)
    noise = jax.random.normal(key_noise, (N2, COLS, N1), jnp.float32)
    lowest = jnp.log(0.1)
    mixed = (second * amplitude[None, :])[:, None, :] * columns[None, :, :]
    signal = jnp.dot(mixed.reshape(N2 * COLS, modes), first.T).reshape(N2, COLS, N1)
    scale_columns = jnp.exp(jax.random.uniform(key_colscale, (COLS,), jnp.float32, lowest, 0.0))
    scale_rows = jnp.exp(jax.random.uniform(key_rowscale, (N2,), jnp.float32, jnp.log(0.5), 0.0))
    values = 4.0 * scale_rows[:, None, None] * scale_columns[None, :, None] * (signal + jnp.sqrt(0.3) * noise)
    return jnp.clip(values, -20.0, 20.0).astype(jnp.float32)


def centred(stream_key, dims, width, bound, held_as=jnp.bfloat16):
    values = width * jax.random.normal(stream_key, dims, jnp.float32)
    return jnp.clip(values, min=-bound, max=bound).astype(held_as)


def setup_inputs(seed: int = 0) -> dict:
    seeds = jax.random.split(jax.random.key(seed), 4)
    return {
        "tensor": draw_tensor(jax.random.fold_in(seeds[3], 71), 0),
        "start_one": centred(seeds[1], (N1, RANK1), 1.0, 6.0, jnp.float32),
        "start_two": centred(seeds[2], (N2, RANK2), 1.0, 6.0, jnp.float32),
    }


HIGH = lax.Precision.HIGHEST

def iterate_basis(gram, start):
    current = start
    for _ in range(ITERS):
        widened = jnp.dot(gram, current, precision=HIGH)
        cross = jnp.dot(widened.T, widened, precision=HIGH)
        lower_small = jnp.linalg.cholesky(cross)
        current = lax.linalg.triangular_solve(lower_small, widened, left_side=False, lower=True, transpose_a=True)
    return current

def reference(tensor, start_one, start_two):
    gram_one = jnp.einsum('jmi,jmk->ik', tensor, tensor, precision=HIGH)
    basis_one = iterate_basis(gram_one, start_one)
    reduced = jnp.einsum('jmi,ia->jma', tensor, basis_one, precision=HIGH)
    gram_two = jnp.einsum('jma,kma->jk', reduced, reduced, precision=HIGH)
    basis_two = iterate_basis(gram_two, start_two)
    core = jnp.einsum('jb,jma->bma', basis_two, reduced, precision=HIGH)
    return (basis_one, basis_two, core)
```

```python
import functools

import jax
import jax.numpy as jnp
from jax import lax
from jax.experimental import pallas as pl
from jax.experimental.pallas import tpu as pltpu
from jax.sharding import PartitionSpec as P

HIGH = lax.Precision.HIGHEST
F32, BF16 = jnp.float32, jnp.bfloat16
LANES = 128
NN = (((1,), (0,)), ((), ()))
NT = (((1,), (1,)), ((), ()))
TN = (((0,), (0,)), ((), ()))
TT = (((0,), (1,)), ((), ()))


def dot(a, b, dims=NN, precision=None):
    return lax.dot_general(a, b, dims, precision=precision, preferred_element_type=F32)


def split(value):
    high = value.astype(BF16)
    low = (value - high.astype(F32)).astype(BF16)
    return high, low


def stacked(value, height):
    high, low = split(value)
    pad = jnp.zeros((height - value.shape[0], value.shape[1]), BF16)
    if pad.shape[0]:
        high, low = (jnp.concatenate([half, pad], axis=0) for half in (high, low))
    return jnp.concatenate([high, low], axis=0)


def ceil_to(value, unit):
    return -(-value // unit) * unit


def packed_rows(rank, wide, devices):
    dense = -(-rank * wide // LANES)
    return devices * ceil_to(-(-dense // devices), 8)


def pack(value, out):
    rank, wide = value.shape
    whole, rest = divmod(wide, LANES)
    for t in range(whole):
        out[t * rank : (t + 1) * rank, :] = value[:, t * LANES : (t + 1) * LANES]
    row = whole * rank
    if rest:
        groups = LANES // rest
        height = rank // groups
        tail = value[:, whole * LANES :]
        out[row : row + height, :] = jnp.concatenate(
            [tail[q * height : (q + 1) * height, :] for q in range(groups)], axis=1
        )
        row += height
    if row < out.shape[0]:
        out[row:, :] = jnp.zeros((out.shape[0] - row, LANES), F32)


def unpack(ref, rank, wide):
    whole, rest = divmod(wide, LANES)
    parts = [ref[t * rank : (t + 1) * rank, :] for t in range(whole)]
    if rest:
        groups = LANES // rest
        height = rank // groups
        tail = ref[whole * rank : whole * rank + height, :]
        parts.append(
            jnp.concatenate([tail[:, q * rest : (q + 1) * rest] for q in range(groups)], axis=0)
        )
    return jnp.concatenate(parts, axis=1)


def cost(flops, moved):
    return pl.CostEstimate(flops=int(flops), bytes_accessed=int(moved), transcendentals=0)


def params():
    return pltpu.CompilerParams(vmem_limit_bytes=32 * 1024 * 1024)


def call(kernel, outs, args, flops, scratch=(), name=None):
    return pl.pallas_call(
        kernel,
        out_shape=outs,
        in_specs=[pl.BlockSpec(memory_space=pltpu.VMEM)] * len(args),
        out_specs=jax.tree.map(lambda _: pl.BlockSpec(memory_space=pltpu.VMEM), outs),
        scratch_shapes=list(scratch),
        compiler_params=params(),
        cost_estimate=cost(flops, sum(a.size * 4 for a in args)),
        name=name,
    )(*args)


def chunk_of(rows):
    return max(c for c in range(16, 513, 16) if rows % c == 0)


def gram_kernel(rank, wide, steps, transposed, x_ref, v_ref, out_ref, vcat, acc):
    step = pl.program_id(0)
    height = vcat.shape[0] // 2

    @pl.when(step == 0)
    def _():
        value = v_ref[...].T if transposed else unpack(v_ref, rank, wide)
        vcat[...] = stacked(value, height)
        acc[...] = jnp.zeros_like(acc)

    xh, xl = split(x_ref[...])
    both = dot(vcat[...], xh, NT)
    z = both[:height] + both[height:] + dot(vcat[:height, :], xl, NT)
    zcat = stacked(z, height)
    both = dot(zcat, xh)
    acc[...] += both[:height] + both[height:] + dot(zcat[:height, :], xl)

    @pl.when(step == steps - 1)
    def _():
        pack(acc[:rank, :], out_ref)


def gram_apply(x, v, rank, rows_out, transposed):
    rows, wide = x.shape
    chunk = chunk_of(rows)
    steps = rows // chunk
    height = ceil_to(rank, LANES)
    return pl.pallas_call(
        functools.partial(gram_kernel, rank, wide, steps, transposed),
        grid=(steps,),
        out_shape=jax.ShapeDtypeStruct((rows_out, LANES), F32),
        in_specs=[
            pl.BlockSpec((chunk, wide), lambda i: (i, 0)),
            pl.BlockSpec(v.shape, lambda i: (0, 0)),
        ],
        out_specs=pl.BlockSpec((rows_out, LANES), lambda i: (0, 0)),
        scratch_shapes=[pltpu.VMEM((2 * height, wide), BF16), pltpu.VMEM((height, wide), F32)],
        compiler_params=params(),
        cost_estimate=cost(12 * rows * wide * rank, 4 * rows * wide),
        name="gram_apply",
    )(x, v)


def project_kernel(rank, wide, cols, groups, x_ref, q_ref, m_ref, w_ref, out_ref, vcat, u):
    step = pl.program_id(0)
    steps = pl.num_programs(0)
    height = vcat.shape[0] // 2
    chunk = x_ref.shape[0]

    @pl.when(step == 0)
    def _():
        w = dot(m_ref[...], unpack(q_ref, rank, wide), precision=HIGH)
        w_ref[...] = w
        vcat[...] = stacked(w, height)

    xh, xl = split(x_ref[...])
    both = dot(xh, vcat[...], NT)
    u[pl.ds(pl.multiple_of(step * chunk, chunk), chunk), :] = (
        both[:, :height] + both[:, height:] + dot(xl, vcat[:height, :], NT)
    )

    @pl.when(step == steps - 1)
    def _():
        depth = u.shape[0] // cols
        per = cols // groups
        for g in range(groups):
            pieces = [u[pl.ds(g * per + k, depth, stride=cols), :][:, :rank] for k in range(per)]
            pack_block(jnp.concatenate(pieces, axis=1), out_ref.at[g])


def block_rows(depth, wide):
    whole, rest = divmod(wide, LANES)
    return whole * depth + (ceil_to(-(-depth // (LANES // rest)), 8) if rest else 0)


def pack_block(value, out):
    depth, wide = value.shape
    whole, rest = divmod(wide, LANES)
    for t in range(whole):
        out[t * depth : (t + 1) * depth, :] = value[:, t * LANES : (t + 1) * LANES]
    if rest:
        fold = LANES // rest
        height = ceil_to(-(-depth // fold), 8)
        tail = value[:, whole * LANES :]
        parts = []
        for q in range(fold):
            part = tail[q * height : min((q + 1) * height, depth), :]
            if part.shape[0] < height:
                part = jnp.concatenate([part, jnp.zeros((height - part.shape[0], rest), F32)], axis=0)
            parts.append(part)
        out[whole * depth :, :] = jnp.concatenate(parts, axis=1)


def unpack_block(ref, depth, wide):
    whole, rest = divmod(wide, LANES)
    parts = [ref[t * depth : (t + 1) * depth, :] for t in range(whole)]
    if rest:
        fold = LANES // rest
        height = ceil_to(-(-depth // fold), 8)
        tail = ref[whole * depth :, :]
        folded = [
            tail[: min(height, depth - q * height), q * rest : (q + 1) * rest] for q in range(fold)
        ]
        parts.append(jnp.concatenate(folded, axis=0))
    return jnp.concatenate(parts, axis=1)


def project(x, q, m, rank, cols, groups):
    rows, wide = x.shape
    chunk = chunk_of(rows)
    height = ceil_to(rank, LANES)
    out_rows = block_rows(rows // cols, (cols // groups) * rank)
    return pl.pallas_call(
        functools.partial(project_kernel, rank, wide, cols, groups),
        grid=(rows // chunk,),
        out_shape=(
            jax.ShapeDtypeStruct((rank, wide), F32),
            jax.ShapeDtypeStruct((groups, out_rows, LANES), F32),
        ),
        in_specs=[
            pl.BlockSpec((chunk, wide), lambda i: (i, 0)),
            pl.BlockSpec(q.shape, lambda i: (0, 0)),
            pl.BlockSpec(m.shape, lambda i: (0, 0)),
        ],
        out_specs=(
            pl.BlockSpec((rank, wide), lambda i: (0, 0)),
            pl.BlockSpec((groups, out_rows, LANES), lambda i: (0, 0, 0)),
        ),
        scratch_shapes=[pltpu.VMEM((2 * height, wide), BF16), pltpu.VMEM((rows, height), F32)],
        compiler_params=params(),
        cost_estimate=cost(6 * rows * wide * rank, 4 * rows * wide),
        name="project",
    )(x, q, m)


def inverse_factor(cross, aug):
    rank = cross.shape[0]
    height, width = aug.shape[0], aug.shape[1] // 2
    row = lax.broadcasted_iota(jnp.int32, (height, width), 0)
    lane = lax.broadcasted_iota(jnp.int32, (height, width), 1)
    eye = (row == lane).astype(F32)
    aug[:, width:] = eye
    aug[:, :width] = eye
    aug[:rank, :rank] = cross
    sub = lax.broadcasted_iota(jnp.int32, (8, 1), 0)
    lane8 = lax.broadcasted_iota(jnp.int32, (8, width), 1)

    def panel(index, carry):
        first = pl.multiple_of(index * 8, 8)
        block = aug[pl.ds(first, 8), :]
        left = block[:, :width]
        columns = [
            jnp.sum(jnp.where(lane8 == first + c, left, 0.0), axis=1, keepdims=True) for c in range(8)
        ]
        pivots = jnp.ones((8, 1), F32)
        for r in range(8):
            pivot = columns[r][r : r + 1, :]
            factor = jnp.where(sub > r, columns[r] / pivot, 0.0)
            pivots = jnp.where(sub == r, pivot, pivots)
            block = block - factor * block[r : r + 1, :]
            for c in range(r + 1, 8):
                columns[c] = columns[c] - factor * columns[c][r : r + 1, :]
        block = block / jnp.sqrt(pivots)
        aug[pl.ds(first, 8), :] = block
        below = jnp.where(lane8 >= first + 8, block[:, :width], 0.0)
        aug[...] -= dot(below, block, TN, precision=HIGH)[:height]
        return carry

    lax.fori_loop(0, -(-rank // 8), panel, 0)
    return aug[:rank, width : width + rank]


def aug_scratch(rank):
    width = ceil_to(rank, LANES)
    return pltpu.VMEM((width, 2 * width), F32)


def factor_packed_kernel(rank, wide, w_ref, m_ref, aug):
    w = unpack(w_ref, rank, wide)
    m_ref[...] = inverse_factor(dot(w, w, NT, precision=HIGH), aug)


def factor_packed(w, rank, wide):
    return call(
        functools.partial(factor_packed_kernel, rank, wide),
        jax.ShapeDtypeStruct((rank, rank), F32),
        (w,),
        3e9,
        [aug_scratch(rank)],
        name="factor_packed",
    )


def factor_basis_kernel(rank, w_ref, m_ref, basis_ref, aug):
    w = w_ref[...]
    m = inverse_factor(dot(w, w, NT, precision=HIGH), aug)
    m_ref[...] = m
    basis_ref[...] = dot(w, m, TT, precision=HIGH)


def factor_basis(w):
    rank, wide = w.shape
    return call(
        functools.partial(factor_basis_kernel, rank),
        (jax.ShapeDtypeStruct((rank, rank), F32), jax.ShapeDtypeStruct((wide, rank), F32)),
        (w,),
        3e9,
        [aug_scratch(rank)],
        name="factor_basis",
    )


def second_kernel(rank, per, depth, u_ref, m_ref, start_ref, y_ref, out_ref):
    groups = u_ref.shape[0]
    for g in range(groups):
        block = unpack_block(u_ref.at[g], depth, per * rank)
        for k in range(per):
            y_ref[k, g * depth : (g + 1) * depth, :] = dot(
                block[:, k * rank : (k + 1) * rank], m_ref[...], NT, precision=HIGH
            )
    total = None
    for k in range(per):
        y = y_ref[k]
        term = dot(dot(start_ref[...], y, TN, precision=HIGH), y, NT, precision=HIGH)
        total = term if total is None else total + term
    pack(total, out_ref)


def second_first(u, m, start, per, rows_out):
    groups = u.shape[0]
    wide, rank2 = start.shape
    rank = m.shape[0]
    return call(
        functools.partial(second_kernel, rank, per, wide // groups),
        (
            jax.ShapeDtypeStruct((per, wide, rank), F32),
            jax.ShapeDtypeStruct((rows_out, LANES), F32),
        ),
        (u, m, start),
        1e8,
        name="second_first",
    )


def second_again_kernel(rank2, wide, y_ref, w_ref, out_ref):
    w = unpack(w_ref, rank2, wide)
    total = None
    for k in range(y_ref.shape[0]):
        y = y_ref[k]
        term = dot(dot(w, y, precision=HIGH), y, NT, precision=HIGH)
        total = term if total is None else total + term
    pack(total, out_ref)


def second_again(y, w, rank2, rows_out):
    return call(
        functools.partial(second_again_kernel, rank2, y.shape[1]),
        jax.ShapeDtypeStruct((rows_out, LANES), F32),
        (y, w),
        1e8,
        name="second_again",
    )


def last_kernel(rank2, wide, q_ref, m_ref, y_ref, basis_ref, core_ref, aug):
    w = dot(m_ref[...], unpack(q_ref, rank2, wide), precision=HIGH)
    m = inverse_factor(dot(w, w, NT, precision=HIGH), aug)
    basis_ref[...] = dot(w, m, TT, precision=HIGH)
    v = dot(m, w, precision=HIGH)
    for k in range(y_ref.shape[0]):
        block = dot(v, y_ref[k], precision=HIGH)
        height = core_ref.shape[2]
        for g in range(core_ref.shape[0]):
            core_ref[g, k] = block[g * height : (g + 1) * height, :]


def last(q, m, y, rank2, groups):
    per, wide, rank = y.shape
    return call(
        functools.partial(last_kernel, rank2, wide),
        (
            jax.ShapeDtypeStruct((wide, rank2), F32),
            jax.ShapeDtypeStruct((groups, per, rank2 // groups, rank), F32),
        ),
        (q, m, y),
        3e9,
        [aug_scratch(rank2)],
        name="last",
    )


def sum_kernel(in_ref, out_ref):
    total = in_ref[0]
    for d in range(1, in_ref.shape[0]):
        total = total + in_ref[d]
    for d in range(in_ref.shape[0]):
        out_ref[d] = total


def total_over(value, axes, devices):
    rows = value.shape[0]
    shares = lax.all_to_all(
        value.reshape(devices, rows // devices, LANES), axes, split_axis=0, concat_axis=0, tiled=True
    )
    copies = call(
        sum_kernel, jax.ShapeDtypeStruct(shares.shape, F32), (shares,), 1e6, name="share_sum"
    )
    whole = lax.all_to_all(copies, axes, split_axis=0, concat_axis=0, tiled=True)
    return whole.reshape(rows, LANES)


def local(groups, slabs, tensor, start_one, start_two):
    axes = ("grp", "slab")
    devices = groups * slabs
    depth, cols, wide = tensor.shape
    rank, rank2 = start_one.shape[1], start_two.shape[1]
    wide2 = start_two.shape[0]
    x = tensor.reshape(depth * cols, wide)
    rows = packed_rows(rank, wide, devices)
    rows2 = packed_rows(rank2, wide2, devices)
    per = cols // groups

    w1 = total_over(gram_apply(x, start_one, rank, rows, True), axes, devices)
    m1 = factor_packed(w1, rank, wide)
    q2 = total_over(gram_apply(x, w1, rank, rows, False), axes, devices)
    w2, u = project(x, q2, m1, rank, cols, groups)
    m2, basis_one = factor_basis(w2)
    u = lax.all_to_all(u, "grp", split_axis=0, concat_axis=0, tiled=True)
    y, p3 = second_first(u, m2, start_two, per, rows2)
    w3 = total_over(p3, axes, devices)
    m3 = factor_packed(w3, rank2, wide2)
    q4 = total_over(second_again(y, w3, rank2, rows2), axes, devices)
    basis_two, core = last(q4, m3, y, rank2, groups)
    core = lax.all_to_all(core, "grp", split_axis=0, concat_axis=0, tiled=True)
    core = core.transpose(2, 0, 1, 3).reshape(rank2 // groups, cols, rank)
    return (basis_one, basis_two, core)


def solution(mesh):
    groups, slabs = mesh.shape["grp"], mesh.shape["slab"]
    in_specs = (P("grp", "slab", None), P(), P())
    out_specs = (P(), P(), P("grp", "slab", None))
    return jax.shard_map(
        functools.partial(local, groups, slabs),
        mesh=mesh,
        in_specs=in_specs,
        out_specs=out_specs,
        check_vma=False,
    )
```

```python
import functools

import jax
import jax.numpy as jnp
from jax import lax
from jax.experimental import pallas as pl
from jax.experimental.pallas import tpu as pltpu
from jax.sharding import PartitionSpec as P

HIGH = lax.Precision.HIGHEST
F32, BF16 = jnp.float32, jnp.bfloat16
LANES = 128
PANEL = 16
NN = (((1,), (0,)), ((), ()))
NT = (((1,), (1,)), ((), ()))
TN = (((0,), (0,)), ((), ()))


def dot(a, b, dims=NN, precision=None):
    return lax.dot_general(a, b, dims, precision=precision, preferred_element_type=F32)


def split(value):
    high = value.astype(BF16)
    low = (value - high.astype(F32)).astype(BF16)
    return high, low


def thirds(value):
    high = value.astype(BF16)
    rest = value - high.astype(F32)
    middle = rest.astype(BF16)
    return high, middle, (rest - middle.astype(F32)).astype(BF16)


def stacked(value, height):
    high, low = split(value)
    pad = jnp.zeros((height - value.shape[0], value.shape[1]), BF16)
    if pad.shape[0]:
        high, low = (jnp.concatenate([half, pad], axis=0) for half in (high, low))
    return jnp.concatenate([high, low], axis=0)


def ceil_to(value, unit):
    return -(-value // unit) * unit


def packed_rows(rank, wide, devices):
    dense = -(-rank * wide // LANES)
    return devices * ceil_to(-(-dense // devices), 8)


def pack(value, out):
    rank, wide = value.shape
    whole, rest = divmod(wide, LANES)
    for t in range(whole):
        out[t * rank : (t + 1) * rank, :] = value[:, t * LANES : (t + 1) * LANES]
    row = whole * rank
    if rest:
        groups = LANES // rest
        height = rank // groups
        tail = value[:, whole * LANES :]
        out[row : row + height, :] = jnp.concatenate(
            [tail[q * height : (q + 1) * height, :] for q in range(groups)], axis=1
        )
        row += height
    if row < out.shape[0]:
        out[row:, :] = jnp.zeros((out.shape[0] - row, LANES), F32)


def unpack(ref, rank, wide):
    whole, rest = divmod(wide, LANES)
    parts = [ref[t * rank : (t + 1) * rank, :] for t in range(whole)]
    if rest:
        groups = LANES // rest
        height = rank // groups
        tail = ref[whole * rank : whole * rank + height, :]
        parts.append(
            jnp.concatenate([tail[:, q * rest : (q + 1) * rest] for q in range(groups)], axis=0)
        )
    return jnp.concatenate(parts, axis=1)


def cost(flops, moved):
    return pl.CostEstimate(flops=int(flops), bytes_accessed=int(moved), transcendentals=0)


def in_hbm(array):
    return pltpu.with_memory_space_constraint(array, pltpu.HBM)


def in_vmem(array):
    return pltpu.with_memory_space_constraint(array, pltpu.VMEM)


def params():
    return pltpu.CompilerParams(vmem_limit_bytes=20 * 1024 * 1024)


def call(kernel, outs, args, flops, scratch=(), name=None, hbm=()):
    return pl.pallas_call(
        kernel,
        out_shape=outs,
        in_specs=[
            pl.BlockSpec(memory_space=pltpu.HBM if i in hbm else pltpu.VMEM) for i in range(len(args))
        ],
        out_specs=jax.tree.map(lambda _: pl.BlockSpec(memory_space=pltpu.VMEM), outs),
        scratch_shapes=list(scratch),
        compiler_params=params(),
        cost_estimate=cost(flops, sum(a.size * 4 for a in args)),
        name=name,
    )(*args)


def chunk_of(rows):
    return max(c for c in range(16, 513, 16) if rows % c == 0)


def gram_chunk(xh, xl, vcat):
    height = vcat.shape[0] // 2
    both = dot(vcat[...], xh, NT)
    z = both[:height] + both[height:] + dot(vcat[:height, :], xl, NT)
    zcat = stacked(z, height)
    both = dot(zcat, xh)
    return both[:height] + both[height:] + dot(zcat[:height, :], xl)


def low_reads(hbm, buffer, sems):
    steps, chunk, _ = buffer.shape
    return [
        pltpu.make_async_copy(hbm.at[pl.ds(i * chunk, chunk), :], buffer.at[i], sems.at[i])
        for i in range(steps)
    ]


def low_scratch(rows, wide):
    chunk = chunk_of(rows)
    return [
        pltpu.VMEM((rows // chunk, chunk, wide), BF16),
        pltpu.SemaphoreType.DMA((rows // chunk,)),
    ]


def gram_first_kernel(x_hbm, v_hbm, out_ref, xh_ref, xl_ref, xbuf, vbuf, vcat, sems):
    steps, chunk, _ = xbuf.shape
    start = pltpu.make_async_copy(v_hbm, vbuf, sems.at[steps])
    start.start()
    copies = [
        pltpu.make_async_copy(x_hbm.at[pl.ds(i * chunk, chunk), :], xbuf.at[i], sems.at[i])
        for i in range(steps)
    ]
    for copy in copies:
        copy.start()
    start.wait()
    vcat[...] = stacked(vbuf[...], vcat.shape[0] // 2)
    total = None
    for i in range(steps):
        copies[i].wait()
        xh, xl = split(xbuf[i])
        xh_ref[i * chunk : (i + 1) * chunk, :] = xh
        xl_ref[i * chunk : (i + 1) * chunk, :] = xl
        term = gram_chunk(xh, xl, vcat)
        total = term if total is None else total + term
    pack(total[: vbuf.shape[0], :], out_ref)


def gram_first(x, v, rows_out):
    rows, wide = x.shape
    rank = v.shape[0]
    chunk = chunk_of(rows)
    height = ceil_to(rank, LANES)
    vmem = pl.BlockSpec(memory_space=pltpu.VMEM)
    hbm = pl.BlockSpec(memory_space=pltpu.HBM)
    return pl.pallas_call(
        gram_first_kernel,
        out_shape=(
            jax.ShapeDtypeStruct((rows_out, LANES), F32),
            pltpu.VMEM((rows, wide), BF16),
            pltpu.VMEM((rows, wide), BF16),
        ),
        in_specs=[hbm, hbm],
        out_specs=(vmem, vmem, vmem),
        scratch_shapes=[
            pltpu.VMEM((rows // chunk, chunk, wide), F32),
            pltpu.VMEM((rank, wide), F32),
            pltpu.VMEM((2 * height, wide), BF16),
            pltpu.SemaphoreType.DMA((rows // chunk + 1,)),
        ],
        compiler_params=params(),
        cost_estimate=cost(12 * rows * wide * rank, 8 * rows * wide),
        name="gram_first",
    )(in_hbm(x), in_hbm(v))


def gram_again_kernel(rank, xh_ref, xl_ref, w_ref, out_ref, vcat):
    rows, wide = xh_ref.shape
    chunk = chunk_of(rows)
    vcat[...] = stacked(unpack(w_ref, rank, wide), vcat.shape[0] // 2)
    total = None
    for i in range(rows // chunk):
        part = slice(i * chunk, (i + 1) * chunk)
        term = gram_chunk(xh_ref[part, :], xl_ref[part, :], vcat)
        total = term if total is None else total + term
    pack(total[:rank, :], out_ref)


def gram_again(xh, xl, w, rank, rows_out):
    rows, wide = xh.shape
    return call(
        functools.partial(gram_again_kernel, rank),
        jax.ShapeDtypeStruct((rows_out, LANES), F32),
        (in_vmem(xh), in_vmem(xl), w),
        12 * rows * wide * rank,
        [pltpu.VMEM((2 * ceil_to(rank, LANES), wide), BF16)],
        name="gram_again",
    )


def project_kernel(rank, cols, xh_ref, xl_hbm, q_ref, m_ref, w_ref, out_ref, vcat, u, lbuf, sems):
    rows, wide = xh_ref.shape
    chunk = chunk_of(rows)
    height = vcat.shape[0] // 2
    reads = low_reads(xl_hbm, lbuf, sems)
    for read in reads:
        read.start()
    w = dot(m_ref[...], unpack(q_ref, rank, wide), precision=HIGH)
    w_ref[...] = w
    vcat[...] = stacked(w, height)
    for i in range(rows // chunk):
        part = slice(i * chunk, (i + 1) * chunk)
        both = dot(xh_ref[part, :], vcat[...], NT)
        u[part, :] = both[:, :height] + both[:, height:]
    for i in range(rows // chunk):
        reads[i].wait()
        u[i * chunk : (i + 1) * chunk, :] += dot(lbuf[i], vcat[:height, :], NT)
    depth = rows // cols
    groups = out_ref.shape[0]
    per = cols // groups
    for g in range(groups):
        pieces = [u[pl.ds(g * per + k, depth, stride=cols), :][:, :rank] for k in range(per)]
        pack_block(jnp.concatenate(pieces, axis=1), out_ref.at[g])


def block_rows(depth, wide):
    whole, rest = divmod(wide, LANES)
    return whole * depth + (ceil_to(-(-depth // (LANES // rest)), 8) if rest else 0)


def pack_block(value, out):
    depth, wide = value.shape
    whole, rest = divmod(wide, LANES)
    for t in range(whole):
        out[t * depth : (t + 1) * depth, :] = value[:, t * LANES : (t + 1) * LANES]
    if rest:
        fold = LANES // rest
        height = ceil_to(-(-depth // fold), 8)
        tail = value[:, whole * LANES :]
        parts = []
        for q in range(fold):
            part = tail[q * height : min((q + 1) * height, depth), :]
            if part.shape[0] < height:
                part = jnp.concatenate([part, jnp.zeros((height - part.shape[0], rest), F32)], axis=0)
            parts.append(part)
        out[whole * depth :, :] = jnp.concatenate(parts, axis=1)


def unpack_block(ref, depth, wide):
    whole, rest = divmod(wide, LANES)
    parts = [ref[t * depth : (t + 1) * depth, :] for t in range(whole)]
    if rest:
        fold = LANES // rest
        height = ceil_to(-(-depth // fold), 8)
        tail = ref[whole * depth :, :]
        folded = [
            tail[: min(height, depth - q * height), q * rest : (q + 1) * rest] for q in range(fold)
        ]
        parts.append(jnp.concatenate(folded, axis=0))
    return jnp.concatenate(parts, axis=1)


def project(xh, xl, q, m, rank, cols, groups):
    rows, wide = xh.shape
    height = ceil_to(rank, LANES)
    out_rows = block_rows(rows // cols, (cols // groups) * rank)
    return call(
        functools.partial(project_kernel, rank, cols),
        (
            jax.ShapeDtypeStruct((rank, wide), F32),
            jax.ShapeDtypeStruct((groups, out_rows, LANES), F32),
        ),
        (in_vmem(xh), in_hbm(xl), q, m),
        6 * rows * wide * rank,
        [pltpu.VMEM((2 * height, wide), BF16), pltpu.VMEM((rows, height), F32)]
        + low_scratch(rows, wide),
        name="project",
        hbm=(1,),
    )


def inverse_factor(cross, aug):
    rank = cross.shape[0]
    height, width = aug.shape[0], aug.shape[1] // 2
    row = lax.broadcasted_iota(jnp.int32, (height, width), 0)
    lane = lax.broadcasted_iota(jnp.int32, (height, width), 1)
    eye = (row == lane).astype(F32)
    aug[:, width:] = eye
    aug[:, :width] = eye
    aug[:rank, :rank] = cross
    sub = lax.broadcasted_iota(jnp.int32, (PANEL, 1), 0)
    lanes = lax.broadcasted_iota(jnp.int32, (PANEL, width), 1)

    def panel(index, carry):
        first = pl.multiple_of(index * PANEL, PANEL)
        block = aug[pl.ds(first, PANEL), :]
        left = block[:, :width]
        columns = [
            jnp.sum(jnp.where(lanes == first + c, left, 0.0), axis=1, keepdims=True)
            for c in range(PANEL)
        ]
        pivots = jnp.ones((PANEL, 1), F32)
        for r in range(PANEL):
            pivot = columns[r][r : r + 1, :]
            factor = jnp.where(sub > r, columns[r] * (1.0 / pivot), 0.0)
            pivots = jnp.where(sub == r, pivot, pivots)
            block = block - factor * block[r : r + 1, :]
            for c in range(r + 1, PANEL):
                columns[c] = columns[c] - factor * columns[c][r : r + 1, :]
        block = block / jnp.sqrt(pivots)
        aug[pl.ds(first, PANEL), :] = block
        below = jnp.where(lanes >= first + PANEL, block[:, :width], 0.0)
        aug[...] -= stacked_product(below, block)[:height]
        return carry

    lax.fori_loop(0, -(-rank // PANEL), panel, 0)
    return aug[:rank, width : width + rank]


def stacked_product(a, b):
    ah, am, al = thirds(a)
    bh, bm, bl = thirds(b)
    return dot(
        jnp.concatenate([ah, ah, am, ah, al, am], axis=0),
        jnp.concatenate([bh, bm, bh, bl, bh, bm], axis=0),
        TN,
    )


def aug_scratch(rank):
    width = ceil_to(rank, LANES)
    return pltpu.VMEM((width, 2 * width), F32)


def factor_packed_kernel(rank, wide, w_ref, m_ref, aug):
    w = unpack(w_ref, rank, wide)
    m_ref[...] = inverse_factor(dot(w, w, NT, precision=HIGH), aug)


def factor_packed(w, rank, wide):
    return call(
        functools.partial(factor_packed_kernel, rank, wide),
        jax.ShapeDtypeStruct((rank, rank), F32),
        (w,),
        3e9,
        [aug_scratch(rank)],
        name="factor_packed",
    )


def factor_basis_kernel(rank, w_ref, m_ref, basis_ref, aug):
    w = w_ref[...]
    m = inverse_factor(dot(w, w, NT, precision=HIGH), aug)
    m_ref[...] = m
    basis_ref[...] = dot(m, w, precision=HIGH)


def factor_basis(w):
    rank, wide = w.shape
    return call(
        functools.partial(factor_basis_kernel, rank),
        (jax.ShapeDtypeStruct((rank, rank), F32), jax.ShapeDtypeStruct((rank, wide), F32)),
        (w,),
        3e9,
        [aug_scratch(rank)],
        name="factor_basis",
    )


def second_product(v, yh, yl):
    height = ceil_to(v.shape[0], 16)
    vcat = stacked(v, height)
    both = dot(vcat, yh)
    z = both[:height] + both[height:] + dot(vcat[:height, :], yl)
    zcat = stacked(z, height)
    both = dot(zcat, yh, NT)
    total = both[:height] + both[height:] + dot(zcat[:height, :], yl, NT)
    return total[: v.shape[0]]


def second_first_kernel(per, depth, u_ref, m_ref, start_ref, yh_ref, yl_ref, out_ref):
    rank = m_ref.shape[0]
    lanes = yh_ref.shape[1] // per
    for g in range(u_ref.shape[0]):
        block = unpack_block(u_ref.at[g], depth, per * rank)
        part = slice(g * depth, (g + 1) * depth)
        for k in range(per):
            y = dot(block[:, k * rank : (k + 1) * rank], m_ref[...], NT, precision=HIGH)
            pad = jnp.zeros((depth, lanes - rank), F32)
            y = jnp.concatenate([y, pad], axis=1) if lanes > rank else y
            high = y.astype(BF16).astype(F32)
            yh_ref[part, k * lanes : (k + 1) * lanes] = high
            yl_ref[part, k * lanes : (k + 1) * lanes] = y - high
    pack(
        second_product(start_ref[...], yh_ref[...].astype(BF16), yl_ref[...].astype(BF16)), out_ref
    )


def second_first(u, m, start, per, rows_out):
    groups = u.shape[0]
    rank2, wide = start.shape
    lanes = ceil_to(m.shape[0], LANES)
    halves = jax.ShapeDtypeStruct((wide, per * lanes), F32)
    return call(
        functools.partial(second_first_kernel, per, wide // groups),
        (halves, halves, jax.ShapeDtypeStruct((rows_out, LANES), F32)),
        (u, m, start),
        1e8,
        name="second_first",
    )


def second_again_kernel(rank2, yh_ref, yl_ref, w_ref, out_ref):
    w = unpack(w_ref, rank2, yh_ref.shape[0])
    pack(second_product(w, yh_ref[...].astype(BF16), yl_ref[...].astype(BF16)), out_ref)


def second_again(yh, yl, w, rank2, rows_out):
    return call(
        functools.partial(second_again_kernel, rank2),
        jax.ShapeDtypeStruct((rows_out, LANES), F32),
        (yh, yl, w),
        1e8,
        name="second_again",
    )


def last_kernel(rank, rank2, q_ref, m_ref, yh_ref, yl_ref, basis_ref, core_ref, aug):
    wide = yh_ref.shape[0]
    w = dot(m_ref[...], unpack(q_ref, rank2, wide), precision=HIGH)
    m = inverse_factor(dot(w, w, NT, precision=HIGH), aug)
    v = dot(m, w, precision=HIGH)
    basis_ref[...] = v
    height = ceil_to(rank2, 16)
    vcat = stacked(v, height)
    yh, yl = yh_ref[...].astype(BF16), yl_ref[...].astype(BF16)
    both = dot(vcat, yh)
    block = both[:height] + both[height:] + dot(vcat[:height, :], yl)
    groups, per, share, _ = core_ref.shape
    lanes = yh.shape[1] // per
    for k in range(per):
        for g in range(groups):
            core_ref[g, k] = block[g * share : (g + 1) * share, k * lanes : k * lanes + rank]


def last(q, m, yh, yl, per, rank, rank2, groups):
    wide = yh.shape[0]
    return call(
        functools.partial(last_kernel, rank, rank2),
        (
            jax.ShapeDtypeStruct((rank2, wide), F32),
            jax.ShapeDtypeStruct((groups, per, rank2 // groups, rank), F32),
        ),
        (q, m, yh, yl),
        3e9,
        [aug_scratch(rank2)],
        name="last",
    )


def sum_kernel(in_ref, out_ref):
    total = in_ref[0]
    for d in range(1, in_ref.shape[0]):
        total = total + in_ref[d]
    for d in range(in_ref.shape[0]):
        out_ref[d] = total


def total_over(value, axes, devices):
    rows = value.shape[0]
    shares = lax.all_to_all(
        value.reshape(devices, rows // devices, LANES), axes, split_axis=0, concat_axis=0, tiled=True
    )
    copies = call(
        sum_kernel, jax.ShapeDtypeStruct(shares.shape, F32), (shares,), 1e6, name="share_sum"
    )
    whole = lax.all_to_all(copies, axes, split_axis=0, concat_axis=0, tiled=True)
    return whole.reshape(rows, LANES)


def local(groups, slabs, tensor, start_one, start_two):
    axes = ("grp", "slab")
    devices = groups * slabs
    depth, cols, wide = tensor.shape
    rank, rank2 = start_one.shape[1], start_two.shape[1]
    wide2 = start_two.shape[0]
    x = tensor.reshape(depth * cols, wide)
    rows = packed_rows(rank, wide, devices)
    rows2 = packed_rows(rank2, wide2, devices)
    per = cols // groups

    p1, xh, xl = gram_first(x, start_one.T, rows)
    w1 = total_over(p1, axes, devices)
    m1 = factor_packed(w1, rank, wide)
    q2 = total_over(gram_again(xh, xl, w1, rank, rows), axes, devices)
    w2, u = project(xh, xl, q2, m1, rank, cols, groups)
    m2, basis_one = factor_basis(w2)
    u = lax.all_to_all(u, "grp", split_axis=0, concat_axis=0, tiled=True)
    yh, yl, p3 = second_first(u, m2, start_two.T, per, rows2)
    w3 = total_over(p3, axes, devices)
    m3 = factor_packed(w3, rank2, wide2)
    q4 = total_over(second_again(yh, yl, w3, rank2, rows2), axes, devices)
    basis_two, core = last(q4, m3, yh, yl, per, rank, rank2, groups)
    core = lax.all_to_all(core, "grp", split_axis=0, concat_axis=0, tiled=True)
    core = core.transpose(2, 0, 1, 3).reshape(rank2 // groups, cols, rank)
    return (basis_one.T, basis_two.T, core)


def solution(mesh):
    groups, slabs = mesh.shape["grp"], mesh.shape["slab"]
    in_specs = (P("grp", "slab", None), P(), P())
    out_specs = (P(), P(), P("grp", "slab", None))
    return jax.shard_map(
        functools.partial(local, groups, slabs),
        mesh=mesh,
        in_specs=in_specs,
        out_specs=out_specs,
        check_vma=False,
    )
```

```python
import functools

import jax
import jax.numpy as jnp
from jax import lax
from jax.experimental import pallas as pl
from jax.experimental.pallas import tpu as pltpu
from jax.sharding import Mesh
from jax.sharding import PartitionSpec as P

HIGH = lax.Precision.HIGHEST
F32, BF16 = jnp.float32, jnp.bfloat16
LANES = 128
PANEL = 16
CORES = 2
NN = (((1,), (0,)), ((), ()))
NT = (((1,), (1,)), ((), ()))
TN = (((0,), (0,)), ((), ()))


def dot(a, b, dims=NN, precision=None):
    return lax.dot_general(a, b, dims, precision=precision, preferred_element_type=F32)


def split(value):
    high = value.astype(BF16)
    low = (value - high.astype(F32)).astype(BF16)
    return high, low


def thirds(value):
    high = value.astype(BF16)
    rest = value - high.astype(F32)
    middle = rest.astype(BF16)
    return high, middle, (rest - middle.astype(F32)).astype(BF16)


def stacked(value, height):
    high, low = split(value)
    pad = jnp.zeros((height - value.shape[0], value.shape[1]), BF16)
    if pad.shape[0]:
        high, low = (jnp.concatenate([half, pad], axis=0) for half in (high, low))
    return jnp.concatenate([high, low], axis=0)


def ceil_to(value, unit):
    return -(-value // unit) * unit


def packed_rows(rank, wide, devices):
    dense = -(-rank * wide // LANES)
    return devices * ceil_to(-(-dense // devices), 8)


def pack(value, out):
    rank, wide = value.shape
    whole, rest = divmod(wide, LANES)
    for t in range(whole):
        out[t * rank : (t + 1) * rank, :] = value[:, t * LANES : (t + 1) * LANES]
    row = whole * rank
    if rest:
        groups = LANES // rest
        height = rank // groups
        tail = value[:, whole * LANES :]
        out[row : row + height, :] = jnp.concatenate(
            [tail[q * height : (q + 1) * height, :] for q in range(groups)], axis=1
        )
        row += height
    if row < out.shape[0]:
        out[row:, :] = jnp.zeros((out.shape[0] - row, LANES), F32)


def unpack(ref, rank, wide):
    whole, rest = divmod(wide, LANES)
    parts = [ref[t * rank : (t + 1) * rank, :] for t in range(whole)]
    if rest:
        groups = LANES // rest
        height = rank // groups
        tail = ref[whole * rank : whole * rank + height, :]
        parts.append(
            jnp.concatenate([tail[:, q * rest : (q + 1) * rest] for q in range(groups)], axis=0)
        )
    return jnp.concatenate(parts, axis=1)


def cost(flops, moved):
    return pl.CostEstimate(flops=int(flops), bytes_accessed=int(moved), transcendentals=0)


def in_hbm(array):
    return pltpu.with_memory_space_constraint(array, pltpu.HBM)


def in_vmem(array):
    return pltpu.with_memory_space_constraint(array, pltpu.VMEM)


def params():
    return pltpu.CompilerParams(vmem_limit_bytes=20 * 1024 * 1024)


def call(kernel, outs, args, flops, scratch=(), name=None, hbm=(), smem=()):
    return pl.pallas_call(
        kernel,
        out_shape=outs,
        in_specs=[
            pl.BlockSpec(
                memory_space=pltpu.HBM if i in hbm else pltpu.SMEM if i in smem else pltpu.VMEM
            )
            for i in range(len(args))
        ],
        out_specs=jax.tree.map(lambda _: pl.BlockSpec(memory_space=pltpu.VMEM), outs),
        scratch_shapes=list(scratch),
        compiler_params=params(),
        cost_estimate=cost(flops, sum(a.size * 4 for a in args)),
        name=name,
    )(*args)


def chunk_of(rows):
    return max(c for c in range(16, 513, 16) if rows % c == 0)


def gram_chunk(xh, xl, vcat):
    height = vcat.shape[0] // 2
    both = dot(vcat[...], xh, NT)
    z = both[:height] + both[height:] + dot(vcat[:height, :], xl, NT)
    zcat = stacked(z, height)
    both = dot(zcat, xh)
    return both[:height] + both[height:] + dot(zcat[:height, :], xl)


def low_reads(hbm, buffer, sems):
    steps, chunk, _ = buffer.shape
    return [
        pltpu.make_async_copy(hbm.at[pl.ds(i * chunk, chunk), :], buffer.at[i], sems.at[i])
        for i in range(steps)
    ]


def low_scratch(rows, wide):
    chunk = chunk_of(rows)
    return [
        pltpu.VMEM((rows // chunk, chunk, wide), BF16),
        pltpu.SemaphoreType.DMA((rows // chunk,)),
    ]


def gram_first_kernel(x_hbm, v_hbm, out_ref, xh_ref, xl_ref, xbuf, vbuf, vcat, sems):
    steps, chunk, _ = xbuf.shape
    start = pltpu.make_async_copy(v_hbm, vbuf, sems.at[steps])
    start.start()
    copies = [
        pltpu.make_async_copy(x_hbm.at[pl.ds(i * chunk, chunk), :], xbuf.at[i], sems.at[i])
        for i in range(steps)
    ]
    for copy in copies:
        copy.start()
    start.wait()
    vcat[...] = stacked(vbuf[...], vcat.shape[0] // 2)
    total = None
    for i in range(steps):
        copies[i].wait()
        xh, xl = split(xbuf[i])
        xh_ref[i * chunk : (i + 1) * chunk, :] = xh
        xl_ref[i * chunk : (i + 1) * chunk, :] = xl
        term = gram_chunk(xh, xl, vcat)
        total = term if total is None else total + term
    pack(total[: vbuf.shape[0], :], out_ref)


def gram_first(x, v, rows_out):
    rows, wide = x.shape
    rank = v.shape[0]
    chunk = chunk_of(rows)
    height = ceil_to(rank, LANES)
    vmem = pl.BlockSpec(memory_space=pltpu.VMEM)
    hbm = pl.BlockSpec(memory_space=pltpu.HBM)
    return pl.pallas_call(
        gram_first_kernel,
        out_shape=(
            jax.ShapeDtypeStruct((rows_out, LANES), F32),
            pltpu.VMEM((rows, wide), BF16),
            pltpu.VMEM((rows, wide), BF16),
        ),
        in_specs=[hbm, hbm],
        out_specs=(vmem, vmem, vmem),
        scratch_shapes=[
            pltpu.VMEM((rows // chunk, chunk, wide), F32),
            pltpu.VMEM((rank, wide), F32),
            pltpu.VMEM((2 * height, wide), BF16),
            pltpu.SemaphoreType.DMA((rows // chunk + 1,)),
        ],
        compiler_params=params(),
        cost_estimate=cost(12 * rows * wide * rank, 8 * rows * wide),
        name="gram_first",
    )(in_hbm(x), in_hbm(v))


def gram_again_kernel(rank, xh_ref, xl_ref, w_ref, out_ref, vcat):
    rows, wide = xh_ref.shape
    chunk = chunk_of(rows)
    vcat[...] = stacked(unpack(w_ref, rank, wide), vcat.shape[0] // 2)
    total = None
    for i in range(rows // chunk):
        part = slice(i * chunk, (i + 1) * chunk)
        term = gram_chunk(xh_ref[part, :], xl_ref[part, :], vcat)
        total = term if total is None else total + term
    pack(total[:rank, :], out_ref)


def gram_again(xh, xl, w, rank, rows_out):
    rows, wide = xh.shape
    return call(
        functools.partial(gram_again_kernel, rank),
        jax.ShapeDtypeStruct((rows_out, LANES), F32),
        (in_vmem(xh), in_vmem(xl), w),
        12 * rows * wide * rank,
        [pltpu.VMEM((2 * ceil_to(rank, LANES), wide), BF16)],
        name="gram_again",
    )


def project_kernel(rank, cols, xh_ref, xl_hbm, q_ref, m_ref, w_ref, out_ref, vcat, u, lbuf, sems):
    rows, wide = xh_ref.shape
    chunk = chunk_of(rows)
    height = vcat.shape[0] // 2
    reads = low_reads(xl_hbm, lbuf, sems)
    for read in reads:
        read.start()
    w = dot(m_ref[...], unpack(q_ref, rank, wide), precision=HIGH)
    w_ref[...] = w
    vcat[...] = stacked(w, height)
    for i in range(rows // chunk):
        part = slice(i * chunk, (i + 1) * chunk)
        both = dot(xh_ref[part, :], vcat[...], NT)
        u[part, :] = both[:, :height] + both[:, height:]
    for i in range(rows // chunk):
        reads[i].wait()
        u[i * chunk : (i + 1) * chunk, :] += dot(lbuf[i], vcat[:height, :], NT)
    depth = rows // cols
    groups = out_ref.shape[0]
    per = cols // groups
    for g in range(groups):
        pieces = [u[pl.ds(g * per + k, depth, stride=cols), :][:, :rank] for k in range(per)]
        pack_block(jnp.concatenate(pieces, axis=1), out_ref.at[g])


def block_rows(depth, wide):
    whole, rest = divmod(wide, LANES)
    return whole * depth + (ceil_to(-(-depth // (LANES // rest)), 8) if rest else 0)


def pack_block(value, out):
    depth, wide = value.shape
    whole, rest = divmod(wide, LANES)
    for t in range(whole):
        out[t * depth : (t + 1) * depth, :] = value[:, t * LANES : (t + 1) * LANES]
    if rest:
        fold = LANES // rest
        height = ceil_to(-(-depth // fold), 8)
        tail = value[:, whole * LANES :]
        parts = []
        for q in range(fold):
            part = tail[q * height : min((q + 1) * height, depth), :]
            if part.shape[0] < height:
                part = jnp.concatenate([part, jnp.zeros((height - part.shape[0], rest), F32)], axis=0)
            parts.append(part)
        out[whole * depth :, :] = jnp.concatenate(parts, axis=1)


def unpack_block(ref, depth, wide):
    whole, rest = divmod(wide, LANES)
    parts = [ref[t * depth : (t + 1) * depth, :] for t in range(whole)]
    if rest:
        fold = LANES // rest
        height = ceil_to(-(-depth // fold), 8)
        tail = ref[whole * depth :, :]
        folded = [
            tail[: min(height, depth - q * height), q * rest : (q + 1) * rest] for q in range(fold)
        ]
        parts.append(jnp.concatenate(folded, axis=0))
    return jnp.concatenate(parts, axis=1)


def project(xh, xl, q, m, rank, cols, groups):
    rows, wide = xh.shape
    height = ceil_to(rank, LANES)
    out_rows = block_rows(rows // cols, (cols // groups) * rank)
    return call(
        functools.partial(project_kernel, rank, cols),
        (
            jax.ShapeDtypeStruct((rank, wide), F32),
            jax.ShapeDtypeStruct((groups, out_rows, LANES), F32),
        ),
        (in_vmem(xh), in_hbm(xl), q, m),
        6 * rows * wide * rank,
        [pltpu.VMEM((2 * height, wide), BF16), pltpu.VMEM((rows, height), F32)]
        + low_scratch(rows, wide),
        name="project",
        hbm=(1,),
    )


def inverse_factor(cross, aug):
    rank = cross.shape[0]
    height, width = aug.shape[0], aug.shape[1] // 2
    row = lax.broadcasted_iota(jnp.int32, (height, width), 0)
    lane = lax.broadcasted_iota(jnp.int32, (height, width), 1)
    eye = (row == lane).astype(F32)
    aug[:, width:] = eye
    aug[:, :width] = eye
    aug[:rank, :rank] = cross
    sub = lax.broadcasted_iota(jnp.int32, (PANEL, 1), 0)
    lanes = lax.broadcasted_iota(jnp.int32, (PANEL, width), 1)

    def panel(index, carry):
        first = pl.multiple_of(index * PANEL, PANEL)
        block = aug[pl.ds(first, PANEL), :]
        left = block[:, :width]
        columns = [
            jnp.sum(jnp.where(lanes == first + c, left, 0.0), axis=1, keepdims=True)
            for c in range(PANEL)
        ]
        pivots = jnp.ones((PANEL, 1), F32)
        for r in range(PANEL):
            pivot = columns[r][r : r + 1, :]
            factor = jnp.where(sub > r, columns[r] * (1.0 / pivot), 0.0)
            pivots = jnp.where(sub == r, pivot, pivots)
            block = block - factor * block[r : r + 1, :]
            for c in range(r + 1, PANEL):
                columns[c] = columns[c] - factor * columns[c][r : r + 1, :]
        block = block / jnp.sqrt(pivots)
        aug[pl.ds(first, PANEL), :] = block
        below = jnp.where(lanes >= first + PANEL, block[:, :width], 0.0)
        aug[...] -= stacked_product(below, block)[:height]
        return carry

    lax.fori_loop(0, -(-rank // PANEL), panel, 0)
    return aug[:rank, width : width + rank]


def stacked_product(a, b):
    ah, am, al = thirds(a)
    bh, bm, bl = thirds(b)
    return dot(
        jnp.concatenate([ah, ah, am, ah, al, am], axis=0),
        jnp.concatenate([bh, bm, bh, bl, bh, bm], axis=0),
        TN,
    )


def aug_scratch(rank):
    width = ceil_to(rank, LANES)
    return pltpu.VMEM((width, 2 * width), F32)


def factor_packed_kernel(rank, wide, w_ref, m_ref, aug):
    w = unpack(w_ref, rank, wide)
    m_ref[...] = inverse_factor(dot(w, w, NT, precision=HIGH), aug)


def factor_packed(w, rank, wide):
    return call(
        functools.partial(factor_packed_kernel, rank, wide),
        jax.ShapeDtypeStruct((rank, rank), F32),
        (w,),
        3e9,
        [aug_scratch(rank)],
        name="factor_packed",
    )


def factor_basis_kernel(rank, w_ref, m_ref, basis_ref, aug):
    w = w_ref[...]
    m = inverse_factor(dot(w, w, NT, precision=HIGH), aug)
    m_ref[...] = m
    basis_ref[...] = dot(m, w, precision=HIGH)


def factor_basis(w):
    rank, wide = w.shape
    return call(
        functools.partial(factor_basis_kernel, rank),
        (jax.ShapeDtypeStruct((rank, rank), F32), jax.ShapeDtypeStruct((rank, wide), F32)),
        (w,),
        3e9,
        [aug_scratch(rank)],
        name="factor_basis",
    )


def merge(whole, core_ref, own, other):
    half = own.shape[0]
    core = core_ref[0]
    whole[pl.ds(pl.multiple_of(core * half, half), half), :] = own
    whole[pl.ds(pl.multiple_of((1 - core) * half, half), half), :] = other


def six_products(a, b, dims):
    height = ceil_to(a.shape[0], 16)
    pad = jnp.zeros((height - a.shape[0], a.shape[1]), BF16)
    parts = thirds(a)
    if pad.shape[0]:
        parts = [jnp.concatenate([part, pad], axis=0) for part in parts]
    three = jnp.concatenate(parts, axis=0)
    first = dot(three, b[0], dims)
    second = dot(three[: 2 * height], b[1], dims)
    third = dot(three[:height], b[2], dims)
    total = (third + first[2 * height :] + second[height:]) + (first[height : 2 * height] + second[:height])
    return (total + first[:height])[: a.shape[0]]


def second_product(v, y):
    return six_products(six_products(v, y, NN), y, NT)


def second_first_kernel(per, depth, core_ref, own_ref, other_ref, m_ref, start_ref, *rest):
    *y_refs, out_ref, buf = rest
    rank = m_ref.shape[0]
    half = start_ref.shape[0] // CORES
    lanes = buf.shape[1] // (CORES * per)
    pad = jnp.zeros((depth, lanes - rank), F32)
    for c, u_ref in enumerate((own_ref, other_ref)):
        for g in range(u_ref.shape[0]):
            block = unpack_block(u_ref.at[g], depth, per * rank)
            for k in range(per):
                u = block[:, k * rank : (k + 1) * rank]
                u = jnp.concatenate([u, pad], axis=1) if lanes > rank else u
                place = (c * per + k) * lanes
                buf[g * depth : (g + 1) * depth, place : place + lanes] = u
    m = m_ref[...]
    if lanes > rank:
        m = jnp.concatenate([m, jnp.zeros((rank, lanes - rank), F32)], axis=1)
        m = jnp.concatenate([m, jnp.zeros((lanes - rank, lanes), F32)], axis=0)
    mt = jnp.concatenate(thirds(m), axis=0)
    uh, um, ul = thirds(buf[...])
    for k in range(CORES * per):
        part = slice(k * lanes, (k + 1) * lanes)
        first = dot(uh[:, part], mt, NT)
        second = dot(um[:, part], mt[: 2 * lanes, :], NT)
        y = first[:, 2 * lanes :] + second[:, lanes:] + dot(ul[:, part], mt[:lanes, :], NT)
        y = y + (first[:, lanes : 2 * lanes] + second[:, :lanes]) + first[:, :lanes]
        for y_ref, third in zip(y_refs, thirds(y)):
            y_ref[:, part] = third
    start = start_ref[pl.ds(pl.multiple_of(core_ref[0] * half, half), half), :]
    pack(second_product(start, [y_ref[...] for y_ref in y_refs]), out_ref)


def second_first(core, own, other, m, start, per, rows_out):
    groups = own.shape[0]
    rank2, wide = start.shape
    columns = CORES * per * ceil_to(m.shape[0], LANES)
    part = jax.ShapeDtypeStruct((wide, columns), BF16)
    *y, out = call(
        functools.partial(second_first_kernel, per, wide // groups),
        (part, part, part, jax.ShapeDtypeStruct((rows_out, LANES), F32)),
        (core, own, other, m, start),
        1e8,
        [pltpu.VMEM((wide, columns), F32)],
        name="second_first",
        smem=(0,),
    )
    return y, out


def second_again_kernel(half, yh_ref, ym_ref, yl_ref, w_ref, out_ref):
    w = unpack(w_ref, half, yh_ref.shape[0])
    pack(second_product(w, [yh_ref[...], ym_ref[...], yl_ref[...]]), out_ref)


def second_again(y, w, half, rows_out):
    return call(
        functools.partial(second_again_kernel, half),
        jax.ShapeDtypeStruct((rows_out, LANES), F32),
        (*y, w),
        1e8,
        name="second_again",
    )


def factor_halves_kernel(half, core_ref, own_ref, other_ref, m_ref, whole, aug):
    wide = whole.shape[1]
    merge(whole, core_ref, unpack(own_ref, half, wide), unpack(other_ref, half, wide))
    w = whole[...]
    m_ref[...] = inverse_factor(dot(w, w, NT, precision=HIGH), aug)


def factor_halves(core, own, other, half, wide):
    rank2 = CORES * half
    return call(
        functools.partial(factor_halves_kernel, half),
        jax.ShapeDtypeStruct((rank2, rank2), F32),
        (core, own, other),
        3e9,
        [pltpu.VMEM((rank2, wide), F32), aug_scratch(rank2)],
        name="factor_halves",
        smem=(0,),
    )


def last_kernel(rank, core_ref, own_ref, other_ref, m_ref, yh_ref, ym_ref, basis_ref, out_ref, whole, aug):
    rank2, wide = whole.shape
    half = rank2 // CORES
    merge(whole, core_ref, unpack(own_ref, half, wide), unpack(other_ref, half, wide))
    w = dot(m_ref[...], whole[...], precision=HIGH)
    m = inverse_factor(dot(w, w, NT, precision=HIGH), aug)
    v = dot(m, w, precision=HIGH)
    basis_ref[...] = v
    height = ceil_to(rank2, 16)
    vcat = stacked(v, height)
    groups, per, share, _ = out_ref.shape
    lanes = yh_ref.shape[1] // (CORES * per)
    both = dot(vcat, yh_ref[:, : per * lanes])
    block = both[:height] + both[height:] + dot(vcat[:height, :], ym_ref[:, : per * lanes])
    for k in range(per):
        for g in range(groups):
            out_ref[g, k] = block[g * share : (g + 1) * share, k * lanes : k * lanes + rank]


def last(core, own, other, m, y, per, rank, groups):
    rank2 = m.shape[0]
    wide = y[0].shape[0]
    return call(
        functools.partial(last_kernel, rank),
        (
            jax.ShapeDtypeStruct((rank2, wide), F32),
            jax.ShapeDtypeStruct((groups, per, rank2 // groups, rank), F32),
        ),
        (core, own, other, m, y[0], y[1]),
        3e9,
        [pltpu.VMEM((rank2, wide), F32), aug_scratch(rank2)],
        name="last",
        smem=(0,),
    )


def sum_kernel(in_ref, out_ref):
    total = in_ref[0]
    for d in range(1, in_ref.shape[0]):
        total = total + in_ref[d]
    for d in range(in_ref.shape[0]):
        out_ref[d] = total


def total_over(value, axes, devices):
    rows = value.shape[0]
    shares = lax.all_to_all(
        value.reshape(devices, rows // devices, LANES), axes, split_axis=0, concat_axis=0, tiled=True
    )
    copies = call(
        sum_kernel, jax.ShapeDtypeStruct(shares.shape, F32), (shares,), 1e6, name="share_sum"
    )
    whole = lax.all_to_all(copies, axes, split_axis=0, concat_axis=0, tiled=True)
    return whole.reshape(rows, LANES)


def local(groups, chips, tensor, start_one, start_two):
    every, alike = ("grp", "chip", "core"), ("grp", "chip")
    devices, partners = groups * chips * CORES, groups * chips
    depth, cols, wide = tensor.shape
    rank, rank2 = start_one.shape[1], start_two.shape[1]
    wide2 = start_two.shape[0]
    x = tensor.reshape(depth * cols, wide)
    half = rank2 // CORES
    rows = packed_rows(rank, wide, devices)
    rows2 = packed_rows(half, wide2, partners)
    per = cols // groups
    core = lax.axis_index("core").reshape(1)

    def swap(value):
        return lax.ppermute(value, "core", [(i, CORES - 1 - i) for i in range(CORES)])

    p1, xh, xl = gram_first(x, start_one.T, rows)
    w1 = total_over(p1, every, devices)
    m1 = factor_packed(w1, rank, wide)
    q2 = total_over(gram_again(xh, xl, w1, rank, rows), every, devices)
    w2, u = project(xh, xl, q2, m1, rank, cols, groups)
    m2, basis_one = factor_basis(w2)
    u = lax.all_to_all(u, "grp", split_axis=0, concat_axis=0, tiled=True)
    u, m2 = lax.optimization_barrier((u, m2))
    y, p3 = second_first(core, u, swap(u), m2, start_two.T, per, rows2)
    w3 = total_over(p3, alike, partners)
    p4, w3_other = lax.optimization_barrier((second_again(y, w3, half, rows2), swap(w3)))
    m3 = factor_halves(core, w3, w3_other, half, wide2)
    q4, m3 = lax.optimization_barrier((total_over(p4, alike, partners), m3))
    basis_two, out = last(core, q4, swap(q4), m3, y, per, rank, groups)
    out = lax.all_to_all(out, "grp", split_axis=0, concat_axis=0, tiled=True)
    out = out.transpose(2, 0, 1, 3).reshape(rank2 // groups, cols, rank)
    return (basis_one.T, basis_two.T, out)


def solution(mesh):
    groups, slabs = mesh.shape["grp"], mesh.shape["slab"]
    chips = slabs // CORES
    fine = Mesh(mesh.devices.reshape(groups, chips, CORES), ("grp", "chip", "core"))
    split_spec = P("grp", ("chip", "core"), None)
    return jax.shard_map(
        functools.partial(local, groups, chips),
        mesh=fine,
        in_specs=(split_spec, P(), P()),
        out_specs=(P(), P(), split_spec),
        check_vma=False,
    )
```

```python
import functools

import jax
import jax.numpy as jnp
from jax import lax
from jax.experimental import pallas as pl
from jax.experimental.pallas import tpu as pltpu
from jax.sharding import Mesh
from jax.sharding import PartitionSpec as P

HIGH = lax.Precision.HIGHEST
F32, BF16 = jnp.float32, jnp.bfloat16
LANES = 128
PANEL = 16
CORES = 2
NN = (((1,), (0,)), ((), ()))
NT = (((1,), (1,)), ((), ()))
TN = (((0,), (0,)), ((), ()))


def dot(a, b, dims=NN, precision=None):
    return lax.dot_general(a, b, dims, precision=precision, preferred_element_type=F32)


def split(value):
    high = value.astype(BF16)
    low = (value - high.astype(F32)).astype(BF16)
    return high, low


def thirds(value):
    high = value.astype(BF16)
    rest = value - high.astype(F32)
    middle = rest.astype(BF16)
    return high, middle, (rest - middle.astype(F32)).astype(BF16)


def stacked(value, height):
    high, low = split(value)
    pad = jnp.zeros((height - value.shape[0], value.shape[1]), BF16)
    if pad.shape[0]:
        high, low = (jnp.concatenate([half, pad], axis=0) for half in (high, low))
    return jnp.concatenate([high, low], axis=0)


def ceil_to(value, unit):
    return -(-value // unit) * unit


def packed_rows(rank, wide, devices):
    dense = -(-rank * wide // LANES)
    return devices * ceil_to(-(-dense // devices), 8)


def pack(value, out):
    rank, wide = value.shape
    whole, rest = divmod(wide, LANES)
    for t in range(whole):
        out[t * rank : (t + 1) * rank, :] = value[:, t * LANES : (t + 1) * LANES]
    row = whole * rank
    if rest:
        groups = LANES // rest
        height = rank // groups
        tail = value[:, whole * LANES :]
        out[row : row + height, :] = jnp.concatenate(
            [tail[q * height : (q + 1) * height, :] for q in range(groups)], axis=1
        )
        row += height
    if row < out.shape[0]:
        out[row:, :] = jnp.zeros((out.shape[0] - row, LANES), F32)


def unpack(ref, rank, wide):
    whole, rest = divmod(wide, LANES)
    parts = [ref[t * rank : (t + 1) * rank, :] for t in range(whole)]
    if rest:
        groups = LANES // rest
        height = rank // groups
        tail = ref[whole * rank : whole * rank + height, :]
        parts.append(
            jnp.concatenate([tail[:, q * rest : (q + 1) * rest] for q in range(groups)], axis=0)
        )
    return jnp.concatenate(parts, axis=1)


def cost(flops, moved):
    return pl.CostEstimate(flops=int(flops), bytes_accessed=int(moved), transcendentals=0)


def in_hbm(array):
    return pltpu.with_memory_space_constraint(array, pltpu.HBM)


def in_vmem(array):
    return pltpu.with_memory_space_constraint(array, pltpu.VMEM)


def params():
    return pltpu.CompilerParams(vmem_limit_bytes=20 * 1024 * 1024)


def call(kernel, outs, args, flops, scratch=(), name=None, hbm=(), smem=()):
    return pl.pallas_call(
        kernel,
        out_shape=outs,
        in_specs=[
            pl.BlockSpec(
                memory_space=pltpu.HBM if i in hbm else pltpu.SMEM if i in smem else pltpu.VMEM
            )
            for i in range(len(args))
        ],
        out_specs=jax.tree.map(lambda _: pl.BlockSpec(memory_space=pltpu.VMEM), outs),
        scratch_shapes=list(scratch),
        compiler_params=params(),
        cost_estimate=cost(flops, sum(a.size * 4 for a in args)),
        name=name,
    )(*args)


def chunk_of(rows):
    return max(c for c in range(16, 513, 16) if rows % c == 0)


def gram_chunk(xh, xl, vcat):
    height = vcat.shape[0] // 2
    both = dot(vcat[...], xh, NT)
    z = both[:height] + both[height:] + dot(vcat[:height, :], xl, NT)
    zcat = stacked(z, height)
    both = dot(zcat, xh)
    return both[:height] + both[height:] + dot(zcat[:height, :], xl)


def low_reads(hbm, buffer, sems):
    steps, chunk, _ = buffer.shape
    return [
        pltpu.make_async_copy(hbm.at[pl.ds(i * chunk, chunk), :], buffer.at[i], sems.at[i])
        for i in range(steps)
    ]


def low_scratch(rows, wide):
    chunk = chunk_of(rows)
    return [
        pltpu.VMEM((rows // chunk, chunk, wide), BF16),
        pltpu.SemaphoreType.DMA((rows // chunk,)),
    ]


def gram_first_kernel(x_hbm, v_hbm, out_ref, xh_ref, xl_ref, xbuf, vbuf, vcat, sems):
    steps, chunk, _ = xbuf.shape
    start = pltpu.make_async_copy(v_hbm, vbuf, sems.at[steps])
    start.start()
    copies = [
        pltpu.make_async_copy(x_hbm.at[pl.ds(i * chunk, chunk), :], xbuf.at[i], sems.at[i])
        for i in range(steps)
    ]
    for copy in copies:
        copy.start()
    start.wait()
    vcat[...] = stacked(vbuf[...], vcat.shape[0] // 2)
    total = None
    for i in range(steps):
        copies[i].wait()
        xh, xl = split(xbuf[i])
        xh_ref[i * chunk : (i + 1) * chunk, :] = xh
        xl_ref[i * chunk : (i + 1) * chunk, :] = xl
        term = gram_chunk(xh, xl, vcat)
        total = term if total is None else total + term
    pack(total[: vbuf.shape[0], :], out_ref)


def gram_first(x, v, rows_out):
    rows, wide = x.shape
    rank = v.shape[0]
    chunk = chunk_of(rows)
    height = ceil_to(rank, LANES)
    vmem = pl.BlockSpec(memory_space=pltpu.VMEM)
    hbm = pl.BlockSpec(memory_space=pltpu.HBM)
    return pl.pallas_call(
        gram_first_kernel,
        out_shape=(
            jax.ShapeDtypeStruct((rows_out, LANES), F32),
            pltpu.VMEM((rows, wide), BF16),
            pltpu.VMEM((rows, wide), BF16),
        ),
        in_specs=[hbm, hbm],
        out_specs=(vmem, vmem, vmem),
        scratch_shapes=[
            pltpu.VMEM((rows // chunk, chunk, wide), F32),
            pltpu.VMEM((rank, wide), F32),
            pltpu.VMEM((2 * height, wide), BF16),
            pltpu.SemaphoreType.DMA((rows // chunk + 1,)),
        ],
        compiler_params=params(),
        cost_estimate=cost(12 * rows * wide * rank, 8 * rows * wide),
        name="gram_first",
    )(in_hbm(x), in_hbm(v))


def gram_again_kernel(rank, xh_ref, xl_ref, w_ref, out_ref, vcat):
    rows, wide = xh_ref.shape
    chunk = chunk_of(rows)
    vcat[...] = stacked(unpack(w_ref, rank, wide), vcat.shape[0] // 2)
    total = None
    for i in range(rows // chunk):
        part = slice(i * chunk, (i + 1) * chunk)
        term = gram_chunk(xh_ref[part, :], xl_ref[part, :], vcat)
        total = term if total is None else total + term
    pack(total[:rank, :], out_ref)


def gram_again(xh, xl, w, rank, rows_out):
    rows, wide = xh.shape
    return call(
        functools.partial(gram_again_kernel, rank),
        jax.ShapeDtypeStruct((rows_out, LANES), F32),
        (in_vmem(xh), in_vmem(xl), w),
        12 * rows * wide * rank,
        [pltpu.VMEM((2 * ceil_to(rank, LANES), wide), BF16)],
        name="gram_again",
    )


def project_kernel(rank, cols, groups, me_ref, xh_ref, xl_hbm, q_ref, m_ref, w_ref, *rest):
    out_refs = rest[:groups]
    vcat, u, lbuf, sems = rest[groups:]
    rows, wide = xh_ref.shape
    chunk = chunk_of(rows)
    height = vcat.shape[0] // 2
    reads = low_reads(xl_hbm, lbuf, sems)
    for read in reads:
        read.start()
    w = dot(m_ref[...], unpack(q_ref, rank, wide), precision=HIGH)
    w_ref[...] = w
    vcat[...] = stacked(w, height)
    for i in range(rows // chunk):
        part = slice(i * chunk, (i + 1) * chunk)
        both = dot(xh_ref[part, :], vcat[...], NT)
        u[part, :] = both[:, :height] + both[:, height:]
    for i in range(rows // chunk):
        reads[i].wait()
        u[i * chunk : (i + 1) * chunk, :] += dot(lbuf[i], vcat[:height, :], NT)
    depth = rows // cols
    per = cols // groups
    for r in range(groups):
        first = peer(me_ref[0], r, groups) * per
        pieces = [u[pl.ds(first + k, depth, stride=cols), :][:, :rank] for k in range(per)]
        pack_block(jnp.concatenate(pieces, axis=1), out_refs[r])


def block_rows(depth, wide):
    whole, rest = divmod(wide, LANES)
    return whole * depth + (ceil_to(-(-depth // (LANES // rest)), 8) if rest else 0)


def pack_block(value, out):
    depth, wide = value.shape
    whole, rest = divmod(wide, LANES)
    for t in range(whole):
        out[t * depth : (t + 1) * depth, :] = value[:, t * LANES : (t + 1) * LANES]
    if rest:
        fold = LANES // rest
        height = ceil_to(-(-depth // fold), 8)
        tail = value[:, whole * LANES :]
        parts = []
        for q in range(fold):
            part = tail[q * height : min((q + 1) * height, depth), :]
            if part.shape[0] < height:
                part = jnp.concatenate([part, jnp.zeros((height - part.shape[0], rest), F32)], axis=0)
            parts.append(part)
        out[whole * depth :, :] = jnp.concatenate(parts, axis=1)


def unpack_block(ref, depth, wide):
    whole, rest = divmod(wide, LANES)
    parts = [ref[t * depth : (t + 1) * depth, :] for t in range(whole)]
    if rest:
        fold = LANES // rest
        height = ceil_to(-(-depth // fold), 8)
        tail = ref[whole * depth :, :]
        folded = [
            tail[: min(height, depth - q * height), q * rest : (q + 1) * rest] for q in range(fold)
        ]
        parts.append(jnp.concatenate(folded, axis=0))
    return jnp.concatenate(parts, axis=1)


def peer(me, step, groups):
    return me ^ step if groups & (groups - 1) == 0 else lax.rem(me + step, groups)


def source(me, step, groups):
    return me ^ step if groups & (groups - 1) == 0 else lax.rem(me + groups - step, groups)


def pairs(step, groups):
    power = groups & (groups - 1) == 0
    return [(g, g ^ step if power else (g + step) % groups) for g in range(groups)]


def project(me, xh, xl, q, m, rank, cols, groups):
    rows, wide = xh.shape
    height = ceil_to(rank, LANES)
    out_rows = block_rows(rows // cols, (cols // groups) * rank)
    w, *blocks = call(
        functools.partial(project_kernel, rank, cols, groups),
        (jax.ShapeDtypeStruct((rank, wide), F32),)
        + (jax.ShapeDtypeStruct((out_rows, LANES), F32),) * groups,
        (me, in_vmem(xh), in_hbm(xl), q, m),
        6 * rows * wide * rank,
        [pltpu.VMEM((2 * height, wide), BF16), pltpu.VMEM((rows, height), F32)]
        + low_scratch(rows, wide),
        name="project",
        hbm=(2,),
        smem=(0,),
    )
    return w, blocks


def inverse_factor(cross, aug):
    rank = cross.shape[0]
    height, width = aug.shape[0], aug.shape[1] // 2
    row = lax.broadcasted_iota(jnp.int32, (height, width), 0)
    lane = lax.broadcasted_iota(jnp.int32, (height, width), 1)
    eye = (row == lane).astype(F32)
    aug[:, width:] = eye
    aug[:, :width] = eye
    aug[:rank, :rank] = cross
    sub = lax.broadcasted_iota(jnp.int32, (PANEL, 1), 0)
    lanes = lax.broadcasted_iota(jnp.int32, (PANEL, width), 1)

    def panel(index, carry):
        first = pl.multiple_of(index * PANEL, PANEL)
        block = aug[pl.ds(first, PANEL), :]
        left = block[:, :width]
        columns = [
            jnp.sum(jnp.where(lanes == first + c, left, 0.0), axis=1, keepdims=True)
            for c in range(PANEL)
        ]
        pivots = jnp.ones((PANEL, 1), F32)
        for r in range(PANEL):
            pivot = columns[r][r : r + 1, :]
            factor = jnp.where(sub > r, columns[r] * (1.0 / pivot), 0.0)
            pivots = jnp.where(sub == r, pivot, pivots)
            block = block - factor * block[r : r + 1, :]
            for c in range(r + 1, PANEL):
                columns[c] = columns[c] - factor * columns[c][r : r + 1, :]
        block = block / jnp.sqrt(pivots)
        aug[pl.ds(first, PANEL), :] = block
        below = jnp.where(lanes >= first + PANEL, block[:, :width], 0.0)
        aug[...] -= stacked_product(below, block)[:height]
        return carry

    lax.fori_loop(0, -(-rank // PANEL), panel, 0)
    return aug[:rank, width : width + rank]


def stacked_product(a, b):
    ah, am, al = thirds(a)
    bh, bm, bl = thirds(b)
    return dot(
        jnp.concatenate([ah, ah, am, ah, al, am], axis=0),
        jnp.concatenate([bh, bm, bh, bl, bh, bm], axis=0),
        TN,
    )


def aug_scratch(rank):
    width = ceil_to(rank, LANES)
    return pltpu.VMEM((width, 2 * width), F32)


def factor_packed_kernel(rank, wide, w_ref, m_ref, aug):
    w = unpack(w_ref, rank, wide)
    m_ref[...] = inverse_factor(dot(w, w, NT, precision=HIGH), aug)


def factor_packed(w, rank, wide):
    return call(
        functools.partial(factor_packed_kernel, rank, wide),
        jax.ShapeDtypeStruct((rank, rank), F32),
        (w,),
        3e9,
        [aug_scratch(rank)],
        name="factor_packed",
    )


def factor_basis_kernel(rank, w_ref, m_ref, basis_ref, aug):
    w = w_ref[...]
    m = inverse_factor(dot(w, w, NT, precision=HIGH), aug)
    m_ref[...] = m
    basis_ref[...] = dot(m, w, precision=HIGH)


def factor_basis(w):
    rank, wide = w.shape
    return call(
        functools.partial(factor_basis_kernel, rank),
        (jax.ShapeDtypeStruct((rank, rank), F32), jax.ShapeDtypeStruct((rank, wide), F32)),
        (w,),
        3e9,
        [aug_scratch(rank)],
        name="factor_basis",
    )


def merge(whole, core_ref, own, other):
    half = own.shape[0]
    core = core_ref[0]
    whole[pl.ds(pl.multiple_of(core * half, half), half), :] = own
    whole[pl.ds(pl.multiple_of((1 - core) * half, half), half), :] = other


def six_products(a, b, dims):
    height = ceil_to(a.shape[0], 16)
    pad = jnp.zeros((height - a.shape[0], a.shape[1]), BF16)
    parts = thirds(a)
    if pad.shape[0]:
        parts = [jnp.concatenate([part, pad], axis=0) for part in parts]
    three = jnp.concatenate(parts, axis=0)
    first = dot(three, b[0], dims)
    second = dot(three[: 2 * height], b[1], dims)
    third = dot(three[:height], b[2], dims)
    total = (third + first[2 * height :] + second[height:]) + (first[height : 2 * height] + second[:height])
    return (total + first[:height])[: a.shape[0]]


def second_product(v, y):
    return six_products(six_products(v, y, NN), y, NT)


def second_first_kernel(per, depth, groups, core_ref, me_ref, m_ref, start_ref, *rest):
    own_refs, other_refs = rest[:groups], rest[groups : 2 * groups]
    *y_refs, out_ref, buf = rest[2 * groups :]
    rank = m_ref.shape[0]
    half = start_ref.shape[0] // CORES
    lanes = buf.shape[1] // (CORES * per)
    pad = jnp.zeros((depth, lanes - rank), F32)
    for c, u_refs in enumerate((own_refs, other_refs)):
        for r in range(groups):
            block = unpack_block(u_refs[r], depth, per * rank)
            first = pl.multiple_of(source(me_ref[0], r, groups) * depth, 8)
            for k in range(per):
                u = block[:, k * rank : (k + 1) * rank]
                u = jnp.concatenate([u, pad], axis=1) if lanes > rank else u
                place = (c * per + k) * lanes
                buf[pl.ds(first, depth), place : place + lanes] = u
    m = m_ref[...]
    if lanes > rank:
        m = jnp.concatenate([m, jnp.zeros((rank, lanes - rank), F32)], axis=1)
        m = jnp.concatenate([m, jnp.zeros((lanes - rank, lanes), F32)], axis=0)
    mt = jnp.concatenate(thirds(m), axis=0)
    uh, um, ul = thirds(buf[...])
    for k in range(CORES * per):
        part = slice(k * lanes, (k + 1) * lanes)
        first = dot(uh[:, part], mt, NT)
        second = dot(um[:, part], mt[: 2 * lanes, :], NT)
        y = first[:, 2 * lanes :] + second[:, lanes:] + dot(ul[:, part], mt[:lanes, :], NT)
        y = y + (first[:, lanes : 2 * lanes] + second[:, :lanes]) + first[:, :lanes]
        for y_ref, third in zip(y_refs, thirds(y)):
            y_ref[:, part] = third
    start = start_ref[pl.ds(pl.multiple_of(core_ref[0] * half, half), half), :]
    pack(second_product(start, [y_ref[...] for y_ref in y_refs]), out_ref)


def second_first(core, me, own, other, m, start, per, rows_out):
    groups = len(own)
    rank2, wide = start.shape
    columns = CORES * per * ceil_to(m.shape[0], LANES)
    part = jax.ShapeDtypeStruct((wide, columns), BF16)
    *y, out = call(
        functools.partial(second_first_kernel, per, wide // groups, groups),
        (part, part, part, jax.ShapeDtypeStruct((rows_out, LANES), F32)),
        (core, me, m, start, *own, *other),
        1e8,
        [pltpu.VMEM((wide, columns), F32)],
        name="second_first",
        smem=(0, 1),
    )
    return y, out


def second_again_kernel(half, yh_ref, ym_ref, yl_ref, w_ref, out_ref):
    w = unpack(w_ref, half, yh_ref.shape[0])
    pack(second_product(w, [yh_ref[...], ym_ref[...], yl_ref[...]]), out_ref)


def second_again(y, w, half, rows_out):
    return call(
        functools.partial(second_again_kernel, half),
        jax.ShapeDtypeStruct((rows_out, LANES), F32),
        (*y, w),
        1e8,
        name="second_again",
    )


def factor_halves_kernel(half, core_ref, own_ref, other_ref, m_ref, whole, aug):
    wide = whole.shape[1]
    merge(whole, core_ref, unpack(own_ref, half, wide), unpack(other_ref, half, wide))
    w = whole[...]
    m_ref[...] = inverse_factor(dot(w, w, NT, precision=HIGH), aug)


def factor_halves(core, own, other, half, wide):
    rank2 = CORES * half
    return call(
        functools.partial(factor_halves_kernel, half),
        jax.ShapeDtypeStruct((rank2, rank2), F32),
        (core, own, other),
        3e9,
        [pltpu.VMEM((rank2, wide), F32), aug_scratch(rank2)],
        name="factor_halves",
        smem=(0,),
    )


def last_kernel(rank, core_ref, own_ref, other_ref, m_ref, yh_ref, ym_ref, basis_ref, out_ref, whole, aug):
    rank2, wide = whole.shape
    half = rank2 // CORES
    merge(whole, core_ref, unpack(own_ref, half, wide), unpack(other_ref, half, wide))
    w = dot(m_ref[...], whole[...], precision=HIGH)
    m = inverse_factor(dot(w, w, NT, precision=HIGH), aug)
    v = dot(m, w, precision=HIGH)
    basis_ref[...] = v
    height = ceil_to(rank2, 16)
    vcat = stacked(v, height)
    groups, per, share, _ = out_ref.shape
    lanes = yh_ref.shape[1] // (CORES * per)
    both = dot(vcat, yh_ref[:, : per * lanes])
    block = both[:height] + both[height:] + dot(vcat[:height, :], ym_ref[:, : per * lanes])
    for k in range(per):
        for g in range(groups):
            out_ref[g, k] = block[g * share : (g + 1) * share, k * lanes : k * lanes + rank]


def last(core, own, other, m, y, per, rank, groups):
    rank2 = m.shape[0]
    wide = y[0].shape[0]
    return call(
        functools.partial(last_kernel, rank),
        (
            jax.ShapeDtypeStruct((rank2, wide), F32),
            jax.ShapeDtypeStruct((groups, per, rank2 // groups, rank), F32),
        ),
        (core, own, other, m, y[0], y[1]),
        3e9,
        [pltpu.VMEM((rank2, wide), F32), aug_scratch(rank2)],
        name="last",
        smem=(0,),
    )


def sum_kernel(in_ref, out_ref):
    total = in_ref[0]
    for d in range(1, in_ref.shape[0]):
        total = total + in_ref[d]
    for d in range(in_ref.shape[0]):
        out_ref[d] = total


def total_over(value, axes, devices):
    rows = value.shape[0]
    shares = lax.all_to_all(
        value.reshape(devices, rows // devices, LANES), axes, split_axis=0, concat_axis=0, tiled=True
    )
    copies = call(
        sum_kernel, jax.ShapeDtypeStruct(shares.shape, F32), (shares,), 1e6, name="share_sum"
    )
    whole = lax.all_to_all(copies, axes, split_axis=0, concat_axis=0, tiled=True)
    return whole.reshape(rows, LANES)


def local(groups, chips, tensor, start_one, start_two):
    every, alike = ("grp", "chip", "core"), ("grp", "chip")
    devices, partners = groups * chips * CORES, groups * chips
    depth, cols, wide = tensor.shape
    rank, rank2 = start_one.shape[1], start_two.shape[1]
    wide2 = start_two.shape[0]
    x = tensor.reshape(depth * cols, wide)
    half = rank2 // CORES
    rows = packed_rows(rank, wide, devices)
    rows2 = packed_rows(half, wide2, partners)
    per = cols // groups
    core, me = lax.axis_index("core").reshape(1), lax.axis_index("grp").reshape(1)

    def swap(value):
        return lax.ppermute(value, "core", [(i, CORES - 1 - i) for i in range(CORES)])

    p1, xh, xl = gram_first(x, start_one.T, rows)
    w1 = total_over(p1, every, devices)
    m1 = factor_packed(w1, rank, wide)
    q2 = total_over(gram_again(xh, xl, w1, rank, rows), every, devices)
    w2, u = project(me, xh, xl, q2, m1, rank, cols, groups)
    m2, basis_one = factor_basis(w2)
    own, other = [u[0]], [swap(u[0])]
    for r in range(1, groups):
        block, m2 = lax.optimization_barrier((lax.ppermute(u[r], "grp", pairs(r, groups)), m2))
        own.append(block)
        other.append(swap(block))
    y, p3 = second_first(core, me, own, other, m2, start_two.T, per, rows2)
    w3 = total_over(p3, alike, partners)
    p4, w3_other = lax.optimization_barrier((second_again(y, w3, half, rows2), swap(w3)))
    m3 = factor_halves(core, w3, w3_other, half, wide2)
    q4, m3 = lax.optimization_barrier((total_over(p4, alike, partners), m3))
    basis_two, out = last(core, q4, swap(q4), m3, y, per, rank, groups)
    out = lax.all_to_all(out, "grp", split_axis=0, concat_axis=0, tiled=True)
    out = out.transpose(2, 0, 1, 3).reshape(rank2 // groups, cols, rank)
    return (basis_one.T, basis_two.T, out)


def solution(mesh):
    groups, slabs = mesh.shape["grp"], mesh.shape["slab"]
    chips = slabs // CORES
    fine = Mesh(mesh.devices.reshape(groups, chips, CORES), ("grp", "chip", "core"))
    split_spec = P("grp", ("chip", "core"), None)
    return jax.shard_map(
        functools.partial(local, groups, chips),
        mesh=fine,
        in_specs=(split_spec, P(), P()),
        out_specs=(P(), P(), split_spec),
        check_vma=False,
    )
```

```python
import functools

import jax
import jax.numpy as jnp
from jax import lax
from jax.experimental import pallas as pl
from jax.experimental.pallas import tpu as pltpu
from jax.sharding import Mesh
from jax.sharding import PartitionSpec as P

HIGH = lax.Precision.HIGHEST
F32, BF16 = jnp.float32, jnp.bfloat16
LANES = 128
PANEL = 16
CORES = 2
NN = (((1,), (0,)), ((), ()))
NT = (((1,), (1,)), ((), ()))
TN = (((0,), (0,)), ((), ()))


def dot(a, b, dims=NN, precision=None):
    return lax.dot_general(a, b, dims, precision=precision, preferred_element_type=F32)


def split(value):
    high = value.astype(BF16)
    low = (value - high.astype(F32)).astype(BF16)
    return high, low


def thirds(value):
    high = value.astype(BF16)
    rest = value - high.astype(F32)
    middle = rest.astype(BF16)
    return high, middle, (rest - middle.astype(F32)).astype(BF16)


def stacked(value, height):
    high, low = split(value)
    pad = jnp.zeros((height - value.shape[0], value.shape[1]), BF16)
    if pad.shape[0]:
        high, low = (jnp.concatenate([half, pad], axis=0) for half in (high, low))
    return jnp.concatenate([high, low], axis=0)


def ceil_to(value, unit):
    return -(-value // unit) * unit


def packed_rows(rank, wide, devices):
    dense = -(-rank * wide // LANES)
    return devices * ceil_to(-(-dense // devices), 8)


def pack(value, out):
    rank, wide = value.shape
    whole, rest = divmod(wide, LANES)
    for t in range(whole):
        out[t * rank : (t + 1) * rank, :] = value[:, t * LANES : (t + 1) * LANES]
    row = whole * rank
    if rest:
        groups = LANES // rest
        height = rank // groups
        tail = value[:, whole * LANES :]
        out[row : row + height, :] = jnp.concatenate(
            [tail[q * height : (q + 1) * height, :] for q in range(groups)], axis=1
        )
        row += height
    if row < out.shape[0]:
        out[row:, :] = jnp.zeros((out.shape[0] - row, LANES), F32)


def unpack(ref, rank, wide):
    whole, rest = divmod(wide, LANES)
    parts = [ref[t * rank : (t + 1) * rank, :] for t in range(whole)]
    if rest:
        groups = LANES // rest
        height = rank // groups
        tail = ref[whole * rank : whole * rank + height, :]
        parts.append(
            jnp.concatenate([tail[:, q * rest : (q + 1) * rest] for q in range(groups)], axis=0)
        )
    return jnp.concatenate(parts, axis=1)


def cost(flops, moved):
    return pl.CostEstimate(flops=int(flops), bytes_accessed=int(moved), transcendentals=0)


def in_hbm(array):
    return pltpu.with_memory_space_constraint(array, pltpu.HBM)


def in_vmem(array):
    return pltpu.with_memory_space_constraint(array, pltpu.VMEM)


def params():
    return pltpu.CompilerParams(vmem_limit_bytes=20 * 1024 * 1024)


def call(kernel, outs, args, flops, scratch=(), name=None, hbm=(), smem=()):
    return pl.pallas_call(
        kernel,
        out_shape=outs,
        in_specs=[
            pl.BlockSpec(
                memory_space=pltpu.HBM if i in hbm else pltpu.SMEM if i in smem else pltpu.VMEM
            )
            for i in range(len(args))
        ],
        out_specs=jax.tree.map(lambda _: pl.BlockSpec(memory_space=pltpu.VMEM), outs),
        scratch_shapes=list(scratch),
        compiler_params=params(),
        cost_estimate=cost(flops, sum(a.size * 4 for a in args)),
        name=name,
    )(*args)


def chunk_of(rows):
    return max(c for c in range(16, 513, 16) if rows % c == 0)


def gram_chunk(xh, xl, vcat):
    height = vcat.shape[0] // 2
    both = dot(vcat[...], xh, NT)
    z = both[:height] + both[height:] + dot(vcat[:height, :], xl, NT)
    zcat = stacked(z, height)
    both = dot(zcat, xh)
    return both[:height] + both[height:] + dot(zcat[:height, :], xl)


def low_reads(hbm, buffer, sems):
    steps, chunk, _ = buffer.shape
    return [
        pltpu.make_async_copy(hbm.at[pl.ds(i * chunk, chunk), :], buffer.at[i], sems.at[i])
        for i in range(steps)
    ]


def low_scratch(rows, wide):
    chunk = chunk_of(rows)
    return [
        pltpu.VMEM((rows // chunk, chunk, wide), BF16),
        pltpu.SemaphoreType.DMA((rows // chunk,)),
    ]


def gram_first_kernel(x_hbm, v_hbm, out_ref, xh_ref, xl_ref, xbuf, vbuf, vcat, sems):
    steps, chunk, _ = xbuf.shape
    start = pltpu.make_async_copy(v_hbm, vbuf, sems.at[steps])
    start.start()
    copies = [
        pltpu.make_async_copy(x_hbm.at[pl.ds(i * chunk, chunk), :], xbuf.at[i], sems.at[i])
        for i in range(steps)
    ]
    for copy in copies:
        copy.start()
    start.wait()
    vcat[...] = stacked(vbuf[...], vcat.shape[0] // 2)
    total = None
    for i in range(steps):
        copies[i].wait()
        xh, xl = split(xbuf[i])
        xh_ref[i * chunk : (i + 1) * chunk, :] = xh
        xl_ref[i * chunk : (i + 1) * chunk, :] = xl
        term = gram_chunk(xh, xl, vcat)
        total = term if total is None else total + term
    pack(total[: vbuf.shape[0], :], out_ref)


def gram_first(x, v, rows_out):
    rows, wide = x.shape
    rank = v.shape[0]
    chunk = chunk_of(rows)
    height = ceil_to(rank, LANES)
    vmem = pl.BlockSpec(memory_space=pltpu.VMEM)
    hbm = pl.BlockSpec(memory_space=pltpu.HBM)
    return pl.pallas_call(
        gram_first_kernel,
        out_shape=(
            jax.ShapeDtypeStruct((rows_out, LANES), F32),
            pltpu.VMEM((rows, wide), BF16),
            pltpu.VMEM((rows, wide), BF16),
        ),
        in_specs=[hbm, hbm],
        out_specs=(vmem, vmem, vmem),
        scratch_shapes=[
            pltpu.VMEM((rows // chunk, chunk, wide), F32),
            pltpu.VMEM((rank, wide), F32),
            pltpu.VMEM((2 * height, wide), BF16),
            pltpu.SemaphoreType.DMA((rows // chunk + 1,)),
        ],
        compiler_params=params(),
        cost_estimate=cost(12 * rows * wide * rank, 8 * rows * wide),
        name="gram_first",
    )(in_hbm(x), in_hbm(v))


def gram_again_kernel(rank, xh_ref, xl_ref, w_ref, out_ref, vcat):
    rows, wide = xh_ref.shape
    chunk = chunk_of(rows)
    vcat[...] = stacked(unpack(w_ref, rank, wide), vcat.shape[0] // 2)
    total = None
    for i in range(rows // chunk):
        part = slice(i * chunk, (i + 1) * chunk)
        term = gram_chunk(xh_ref[part, :], xl_ref[part, :], vcat)
        total = term if total is None else total + term
    pack(total[:rank, :], out_ref)


def gram_again(xh, xl, w, rank, rows_out):
    rows, wide = xh.shape
    return call(
        functools.partial(gram_again_kernel, rank),
        jax.ShapeDtypeStruct((rows_out, LANES), F32),
        (in_vmem(xh), in_vmem(xl), w),
        12 * rows * wide * rank,
        [pltpu.VMEM((2 * ceil_to(rank, LANES), wide), BF16)],
        name="gram_again",
    )


def project_kernel(rank, cols, groups, me_ref, xh_ref, xl_hbm, q_ref, m_ref, w_ref, *rest):
    out_refs = rest[:groups]
    vcat, u, lbuf, sems = rest[groups:]
    rows, wide = xh_ref.shape
    chunk = chunk_of(rows)
    height = vcat.shape[0] // 2
    reads = low_reads(xl_hbm, lbuf, sems)
    for read in reads:
        read.start()
    w = dot(m_ref[...], unpack(q_ref, rank, wide), precision=HIGH)
    w_ref[...] = w
    vcat[...] = stacked(w, height)
    for i in range(rows // chunk):
        part = slice(i * chunk, (i + 1) * chunk)
        both = dot(xh_ref[part, :], vcat[...], NT)
        u[part, :] = both[:, :height] + both[:, height:]
    for i in range(rows // chunk):
        reads[i].wait()
        u[i * chunk : (i + 1) * chunk, :] += dot(lbuf[i], vcat[:height, :], NT)
    depth = rows // cols
    per = cols // groups
    for r in range(groups):
        first = peer(me_ref[0], r, groups) * per
        pieces = [u[pl.ds(first + k, depth, stride=cols), :][:, :rank] for k in range(per)]
        pack_block(jnp.concatenate(pieces, axis=1), out_refs[r])


def block_rows(depth, wide):
    whole, rest = divmod(wide, LANES)
    return whole * depth + (ceil_to(-(-depth // (LANES // rest)), 8) if rest else 0)


def pack_block(value, out):
    depth, wide = value.shape
    whole, rest = divmod(wide, LANES)
    for t in range(whole):
        out[t * depth : (t + 1) * depth, :] = value[:, t * LANES : (t + 1) * LANES]
    if rest:
        fold = LANES // rest
        height = ceil_to(-(-depth // fold), 8)
        tail = value[:, whole * LANES :]
        parts = []
        for q in range(fold):
            part = tail[q * height : min((q + 1) * height, depth), :]
            if part.shape[0] < height:
                part = jnp.concatenate([part, jnp.zeros((height - part.shape[0], rest), F32)], axis=0)
            parts.append(part)
        out[whole * depth :, :] = jnp.concatenate(parts, axis=1)


def unpack_block(ref, depth, wide):
    whole, rest = divmod(wide, LANES)
    parts = [ref[t * depth : (t + 1) * depth, :] for t in range(whole)]
    if rest:
        fold = LANES // rest
        height = ceil_to(-(-depth // fold), 8)
        tail = ref[whole * depth :, :]
        folded = [
            tail[: min(height, depth - q * height), q * rest : (q + 1) * rest] for q in range(fold)
        ]
        parts.append(jnp.concatenate(folded, axis=0))
    return jnp.concatenate(parts, axis=1)


def peer(me, step, groups):
    return me ^ step if groups & (groups - 1) == 0 else lax.rem(me + step, groups)


def source(me, step, groups):
    return me ^ step if groups & (groups - 1) == 0 else lax.rem(me + groups - step, groups)


def pairs(step, groups):
    power = groups & (groups - 1) == 0
    return [(g, g ^ step if power else (g + step) % groups) for g in range(groups)]


def project(me, xh, xl, q, m, rank, cols, groups):
    rows, wide = xh.shape
    height = ceil_to(rank, LANES)
    out_rows = block_rows(rows // cols, (cols // groups) * rank)
    w, *blocks = call(
        functools.partial(project_kernel, rank, cols, groups),
        (jax.ShapeDtypeStruct((rank, wide), F32),)
        + (jax.ShapeDtypeStruct((out_rows, LANES), F32),) * groups,
        (me, in_vmem(xh), in_hbm(xl), q, m),
        6 * rows * wide * rank,
        [pltpu.VMEM((2 * height, wide), BF16), pltpu.VMEM((rows, height), F32)]
        + low_scratch(rows, wide),
        name="project",
        hbm=(2,),
        smem=(0,),
    )
    return w, blocks


def inverse_factor(cross, aug):
    rank = cross.shape[0]
    height, width = aug.shape[0], aug.shape[1] // 2
    row = lax.broadcasted_iota(jnp.int32, (height, width), 0)
    lane = lax.broadcasted_iota(jnp.int32, (height, width), 1)
    eye = (row == lane).astype(F32)
    aug[:, width:] = eye
    aug[:, :width] = eye
    aug[:rank, :rank] = cross
    sub = lax.broadcasted_iota(jnp.int32, (PANEL, 1), 0)
    lanes = lax.broadcasted_iota(jnp.int32, (PANEL, width), 1)

    def panel(index, carry):
        first = pl.multiple_of(index * PANEL, PANEL)
        block = aug[pl.ds(first, PANEL), :]
        left = block[:, :width]
        columns = [
            jnp.sum(jnp.where(lanes == first + c, left, 0.0), axis=1, keepdims=True)
            for c in range(PANEL)
        ]
        pivots = jnp.ones((PANEL, 1), F32)
        for r in range(PANEL):
            pivot = columns[r][r : r + 1, :]
            factor = jnp.where(sub > r, columns[r] * (1.0 / pivot), 0.0)
            pivots = jnp.where(sub == r, pivot, pivots)
            block = block - factor * block[r : r + 1, :]
            for c in range(r + 1, PANEL):
                columns[c] = columns[c] - factor * columns[c][r : r + 1, :]
        block = block / jnp.sqrt(pivots)
        aug[pl.ds(first, PANEL), :] = block
        below = jnp.where(lanes >= first + PANEL, block[:, :width], 0.0)
        aug[...] -= stacked_product(below, block)[:height]
        return carry

    lax.fori_loop(0, -(-rank // PANEL), panel, 0)
    return aug[:rank, width : width + rank]


def stacked_product(a, b):
    ah, am, al = thirds(a)
    bh, bm, bl = thirds(b)
    return dot(
        jnp.concatenate([ah, ah, am, ah, al, am], axis=0),
        jnp.concatenate([bh, bm, bh, bl, bh, bm], axis=0),
        TN,
    )


def aug_scratch(rank):
    width = ceil_to(rank, LANES)
    return pltpu.VMEM((width, 2 * width), F32)


def factor_packed_kernel(rank, wide, w_ref, m_ref, aug):
    w = unpack(w_ref, rank, wide)
    m_ref[...] = inverse_factor(dot(w, w, NT, precision=HIGH), aug)


def factor_packed(w, rank, wide):
    return call(
        functools.partial(factor_packed_kernel, rank, wide),
        jax.ShapeDtypeStruct((rank, rank), F32),
        (w,),
        3e9,
        [aug_scratch(rank)],
        name="factor_packed",
    )


def factor_basis_kernel(rank, w_ref, m_ref, basis_ref, aug):
    w = w_ref[...]
    m = inverse_factor(dot(w, w, NT, precision=HIGH), aug)
    m_ref[...] = m
    basis_ref[...] = dot(m, w, precision=HIGH)


def factor_basis(w):
    rank, wide = w.shape
    return call(
        functools.partial(factor_basis_kernel, rank),
        (jax.ShapeDtypeStruct((rank, rank), F32), jax.ShapeDtypeStruct((rank, wide), F32)),
        (w,),
        3e9,
        [aug_scratch(rank)],
        name="factor_basis",
    )


def merge(whole, core_ref, own, other):
    half = own.shape[0]
    core = core_ref[0]
    whole[pl.ds(pl.multiple_of(core * half, half), half), :] = own
    whole[pl.ds(pl.multiple_of((1 - core) * half, half), half), :] = other


def six_products(a, b, dims):
    height = ceil_to(a.shape[0], 16)
    pad = jnp.zeros((height - a.shape[0], a.shape[1]), BF16)
    parts = thirds(a)
    if pad.shape[0]:
        parts = [jnp.concatenate([part, pad], axis=0) for part in parts]
    three = jnp.concatenate(parts, axis=0)
    first = dot(three, b[0], dims)
    second = dot(three[: 2 * height], b[1], dims)
    third = dot(three[:height], b[2], dims)
    total = (third + first[2 * height :] + second[height:]) + (first[height : 2 * height] + second[:height])
    return (total + first[:height])[: a.shape[0]]


def second_product(v, y):
    return six_products(six_products(v, y, NN), y, NT)


def second_first_kernel(per, depth, groups, core_ref, me_ref, m_ref, start_ref, *rest):
    own_refs, other_refs = rest[:groups], rest[groups : 2 * groups]
    *y_refs, out_ref, buf = rest[2 * groups :]
    rank = m_ref.shape[0]
    half = start_ref.shape[0] // CORES
    lanes = buf.shape[1] // (CORES * per)
    pad = jnp.zeros((depth, lanes - rank), F32)
    for c, u_refs in enumerate((own_refs, other_refs)):
        for r in range(groups):
            block = unpack_block(u_refs[r], depth, per * rank)
            first = pl.multiple_of(source(me_ref[0], r, groups) * depth, 8)
            for k in range(per):
                u = block[:, k * rank : (k + 1) * rank]
                u = jnp.concatenate([u, pad], axis=1) if lanes > rank else u
                place = (c * per + k) * lanes
                buf[pl.ds(first, depth), place : place + lanes] = u
    m = m_ref[...]
    if lanes > rank:
        m = jnp.concatenate([m, jnp.zeros((rank, lanes - rank), F32)], axis=1)
        m = jnp.concatenate([m, jnp.zeros((lanes - rank, lanes), F32)], axis=0)
    mt = stacked(m, lanes)
    uh, ul = split(buf[...])
    for k in range(CORES * per):
        part = slice(k * lanes, (k + 1) * lanes)
        both = dot(uh[:, part], mt, NT)
        y = both[:, :lanes] + (both[:, lanes:] + dot(ul[:, part], mt[:lanes, :], NT))
        for y_ref, third in zip(y_refs, thirds(y)):
            y_ref[:, part] = third
    start = start_ref[pl.ds(pl.multiple_of(core_ref[0] * half, half), half), :]
    pack(second_product(start, [y_ref[...] for y_ref in y_refs]), out_ref)


def second_first(core, me, own, other, m, start, per, rows_out):
    groups = len(own)
    rank2, wide = start.shape
    columns = CORES * per * ceil_to(m.shape[0], LANES)
    part = jax.ShapeDtypeStruct((wide, columns), BF16)
    *y, out = call(
        functools.partial(second_first_kernel, per, wide // groups, groups),
        (part, part, part, jax.ShapeDtypeStruct((rows_out, LANES), F32)),
        (core, me, m, start, *own, *other),
        1e8,
        [pltpu.VMEM((wide, columns), F32)],
        name="second_first",
        smem=(0, 1),
    )
    return y, out


def second_again_kernel(half, yh_ref, ym_ref, yl_ref, w_ref, out_ref):
    w = unpack(w_ref, half, yh_ref.shape[0])
    pack(second_product(w, [yh_ref[...], ym_ref[...], yl_ref[...]]), out_ref)


def second_again(y, w, half, rows_out):
    return call(
        functools.partial(second_again_kernel, half),
        jax.ShapeDtypeStruct((rows_out, LANES), F32),
        (*y, w),
        1e8,
        name="second_again",
    )


def factor_halves_kernel(half, core_ref, own_ref, other_ref, m_ref, whole, aug):
    wide = whole.shape[1]
    merge(whole, core_ref, unpack(own_ref, half, wide), unpack(other_ref, half, wide))
    w = whole[...]
    m_ref[...] = inverse_factor(dot(w, w, NT, precision=HIGH), aug)


def factor_halves(core, own, other, half, wide):
    rank2 = CORES * half
    return call(
        functools.partial(factor_halves_kernel, half),
        jax.ShapeDtypeStruct((rank2, rank2), F32),
        (core, own, other),
        3e9,
        [pltpu.VMEM((rank2, wide), F32), aug_scratch(rank2)],
        name="factor_halves",
        smem=(0,),
    )


def widen_kernel(rank, per, core_ref, own_ref, other_ref, m_ref, yh_ref, ym_ref, yl_ref, w_ref, out_ref, whole):
    rank2, wide = whole.shape
    half = rank2 // CORES
    merge(whole, core_ref, unpack(own_ref, half, wide), unpack(other_ref, half, wide))
    w = dot(m_ref[...], whole[...], precision=HIGH)
    w_ref[...] = w
    lanes = yh_ref.shape[1] // (CORES * per)
    y = [ref[:, : per * lanes] for ref in (yh_ref, ym_ref, yl_ref)]
    block = six_products(w, y, NN)
    pack_block(jnp.concatenate([block[:, k * lanes : k * lanes + rank] for k in range(per)], axis=1), out_ref)


def widen(core, own, other, m, y, per, rank):
    rank2 = m.shape[0]
    wide = y[0].shape[0]
    return call(
        functools.partial(widen_kernel, rank, per),
        (
            jax.ShapeDtypeStruct((rank2, wide), F32),
            jax.ShapeDtypeStruct((block_rows(rank2, per * rank), LANES), F32),
        ),
        (core, own, other, m, *y),
        1e8,
        [pltpu.VMEM((rank2, wide), F32)],
        name="widen",
        smem=(0,),
    )


def core_kernel(rank, per, groups, me_ref, m_ref, *rest):
    block_refs, (out_ref,) = rest[:groups], rest[groups:]
    share = out_ref.shape[0]
    rank2 = m_ref.shape[1]
    mine = m_ref[pl.ds(pl.multiple_of(me_ref[0] * share, 8), share), :]
    for r in range(groups):
        block = dot(mine, unpack_block(block_refs[r], rank2, per * rank), precision=HIGH)
        first = source(me_ref[0], r, groups) * per
        for k in range(per):
            out_ref[:, pl.ds(first + k, 1), :] = block[:, k * rank : (k + 1) * rank].reshape(share, 1, rank)


def core_blocks(me, m, blocks, per, rank):
    groups = len(blocks)
    return call(
        functools.partial(core_kernel, rank, per, groups),
        jax.ShapeDtypeStruct((m.shape[0] // groups, groups * per, rank), F32),
        (me, m, *blocks),
        1e8,
        name="core_blocks",
        smem=(0,),
    )


def sum_kernel(in_ref, out_ref):
    total = in_ref[0]
    for d in range(1, in_ref.shape[0]):
        total = total + in_ref[d]
    for d in range(in_ref.shape[0]):
        out_ref[d] = total


def total_over(value, axes, devices):
    rows = value.shape[0]
    shares = lax.all_to_all(
        value.reshape(devices, rows // devices, LANES), axes, split_axis=0, concat_axis=0, tiled=True
    )
    copies = call(
        sum_kernel, jax.ShapeDtypeStruct(shares.shape, F32), (shares,), 1e6, name="share_sum"
    )
    whole = lax.all_to_all(copies, axes, split_axis=0, concat_axis=0, tiled=True)
    return whole.reshape(rows, LANES)


def local(groups, chips, tensor, start_one, start_two):
    every, alike = ("grp", "chip", "core"), ("grp", "chip")
    devices, partners = groups * chips * CORES, groups * chips
    depth, cols, wide = tensor.shape
    rank, rank2 = start_one.shape[1], start_two.shape[1]
    wide2 = start_two.shape[0]
    x = tensor.reshape(depth * cols, wide)
    half = rank2 // CORES
    rows = packed_rows(rank, wide, devices)
    rows2 = packed_rows(half, wide2, partners)
    per = cols // groups
    core, me = lax.axis_index("core").reshape(1), lax.axis_index("grp").reshape(1)

    def swap(value):
        return lax.ppermute(value, "core", [(i, CORES - 1 - i) for i in range(CORES)])

    p1, xh, xl = gram_first(x, start_one.T, rows)
    w1 = total_over(p1, every, devices)
    m1 = factor_packed(w1, rank, wide)
    q2 = total_over(gram_again(xh, xl, w1, rank, rows), every, devices)
    w2, u = project(me, xh, xl, q2, m1, rank, cols, groups)
    m2, basis_one = factor_basis(w2)
    own, other = [u[0]], [swap(u[0])]
    for r in range(1, groups):
        block, m2 = lax.optimization_barrier((lax.ppermute(u[r], "grp", pairs(r, groups)), m2))
        own.append(block)
        other.append(swap(block))
    y, p3 = second_first(core, me, own, other, m2, start_two.T, per, rows2)
    w3 = total_over(p3, alike, partners)
    p4, w3_other = lax.optimization_barrier((second_again(y, w3, half, rows2), swap(w3)))
    m3 = factor_halves(core, w3, w3_other, half, wide2)
    q4, m3 = lax.optimization_barrier((total_over(p4, alike, partners), m3))
    w4, mixed = widen(core, q4, swap(q4), m3, y, per, rank)
    m4, basis_two = factor_basis(w4)
    blocks = [mixed]
    for r in range(1, groups):
        block, m4 = lax.optimization_barrier((lax.ppermute(mixed, "grp", pairs(r, groups)), m4))
        blocks.append(block)
    out = core_blocks(me, m4, blocks, per, rank)
    return (basis_one.T, basis_two.T, out)


def solution(mesh):
    groups, slabs = mesh.shape["grp"], mesh.shape["slab"]
    chips = slabs // CORES
    fine = Mesh(mesh.devices.reshape(groups, chips, CORES), ("grp", "chip", "core"))
    split_spec = P("grp", ("chip", "core"), None)
    return jax.shard_map(
        functools.partial(local, groups, chips),
        mesh=fine,
        in_specs=(split_spec, P(), P()),
        out_specs=(P(), P(), split_spec),
        check_vma=False,
    )
```

```python
import functools

import jax
import jax.numpy as jnp
from jax import lax
from jax.experimental import pallas as pl
from jax.experimental.pallas import tpu as pltpu
from jax.sharding import Mesh
from jax.sharding import PartitionSpec as P

HIGH = lax.Precision.HIGHEST
F32, BF16 = jnp.float32, jnp.bfloat16
LANES = 128
PANEL = 16
CORES = 2
NN = (((1,), (0,)), ((), ()))
NT = (((1,), (1,)), ((), ()))
TN = (((0,), (0,)), ((), ()))


def dot(a, b, dims=NN, precision=None):
    return lax.dot_general(a, b, dims, precision=precision, preferred_element_type=F32)


def split(value):
    high = value.astype(BF16)
    low = (value - high.astype(F32)).astype(BF16)
    return high, low


def thirds(value):
    high = value.astype(BF16)
    rest = value - high.astype(F32)
    middle = rest.astype(BF16)
    return high, middle, (rest - middle.astype(F32)).astype(BF16)


def stacked(value, height):
    high, low = split(value)
    pad = jnp.zeros((height - value.shape[0], value.shape[1]), BF16)
    if pad.shape[0]:
        high, low = (jnp.concatenate([half, pad], axis=0) for half in (high, low))
    return jnp.concatenate([high, low], axis=0)


def ceil_to(value, unit):
    return -(-value // unit) * unit


def packed_rows(rank, wide, devices):
    dense = -(-rank * wide // LANES)
    return devices * ceil_to(-(-dense // devices), 8)


def pack(value, out):
    rank, wide = value.shape
    whole, rest = divmod(wide, LANES)
    for t in range(whole):
        out[t * rank : (t + 1) * rank, :] = value[:, t * LANES : (t + 1) * LANES]
    row = whole * rank
    if rest:
        groups = LANES // rest
        height = rank // groups
        tail = value[:, whole * LANES :]
        out[row : row + height, :] = jnp.concatenate(
            [tail[q * height : (q + 1) * height, :] for q in range(groups)], axis=1
        )
        row += height
    if row < out.shape[0]:
        out[row:, :] = jnp.zeros((out.shape[0] - row, LANES), F32)


def unpack(ref, rank, wide):
    whole, rest = divmod(wide, LANES)
    parts = [ref[t * rank : (t + 1) * rank, :] for t in range(whole)]
    if rest:
        groups = LANES // rest
        height = rank // groups
        tail = ref[whole * rank : whole * rank + height, :]
        parts.append(
            jnp.concatenate([tail[:, q * rest : (q + 1) * rest] for q in range(groups)], axis=0)
        )
    return jnp.concatenate(parts, axis=1)


def merge(whole, core_ref, own, other):
    half = own.shape[0]
    core = core_ref[0]
    whole[pl.ds(pl.multiple_of(core * half, half), half), :] = own
    whole[pl.ds(pl.multiple_of((1 - core) * half, half), half), :] = other


def cost(flops, moved):
    return pl.CostEstimate(flops=int(flops), bytes_accessed=int(moved), transcendentals=0)


def in_hbm(array):
    return pltpu.with_memory_space_constraint(array, pltpu.HBM)


def in_vmem(array):
    return pltpu.with_memory_space_constraint(array, pltpu.VMEM)


def params():
    return pltpu.CompilerParams(vmem_limit_bytes=20 * 1024 * 1024)


def call(kernel, outs, args, flops, scratch=(), name=None, hbm=(), smem=()):
    return pl.pallas_call(
        kernel,
        out_shape=outs,
        in_specs=[
            pl.BlockSpec(
                memory_space=pltpu.HBM if i in hbm else pltpu.SMEM if i in smem else pltpu.VMEM
            )
            for i in range(len(args))
        ],
        out_specs=jax.tree.map(lambda _: pl.BlockSpec(memory_space=pltpu.VMEM), outs),
        scratch_shapes=list(scratch),
        compiler_params=params(),
        cost_estimate=cost(flops, sum(a.size * 4 for a in args)),
        name=name,
    )(*args)


def chunk_of(rows):
    return max(c for c in range(16, 513, 16) if rows % c == 0)


def gram_chunk(xh, xl, vcat):
    height = vcat.shape[0] // 2
    both = dot(vcat[...], xh, NT)
    z = both[:height] + both[height:] + dot(vcat[:height, :], xl, NT)
    zcat = stacked(z, height)
    both = dot(zcat, xh)
    return both[:height] + both[height:] + dot(zcat[:height, :], xl)


def gram_first_kernel(x_hbm, v_hbm, out_ref, xh_ref, xl_ref, xbuf, vbuf, vcat, sems):
    steps, chunk, _ = xbuf.shape
    start = pltpu.make_async_copy(v_hbm, vbuf, sems.at[steps])
    start.start()
    copies = [
        pltpu.make_async_copy(x_hbm.at[pl.ds(i * chunk, chunk), :], xbuf.at[i], sems.at[i])
        for i in range(steps)
    ]
    for copy in copies:
        copy.start()
    start.wait()
    vcat[...] = stacked(vbuf[...], vcat.shape[0] // 2)
    total = None
    for i in range(steps):
        copies[i].wait()
        xh, xl = split(xbuf[i])
        xh_ref[i * chunk : (i + 1) * chunk, :] = xh
        xl_ref[i * chunk : (i + 1) * chunk, :] = xl
        term = gram_chunk(xh, xl, vcat)
        total = term if total is None else total + term
    pack(total[: vbuf.shape[0], :], out_ref)


def gram_first(x, v, rows_out):
    rows, wide = x.shape
    rank = v.shape[0]
    chunk = chunk_of(rows)
    height = ceil_to(rank, LANES)
    vmem = pl.BlockSpec(memory_space=pltpu.VMEM)
    hbm = pl.BlockSpec(memory_space=pltpu.HBM)
    return pl.pallas_call(
        gram_first_kernel,
        out_shape=(
            jax.ShapeDtypeStruct((rows_out, LANES), F32),
            pltpu.VMEM((rows, wide), BF16),
            pltpu.VMEM((rows, wide), BF16),
        ),
        in_specs=[hbm, hbm],
        out_specs=(vmem, vmem, vmem),
        scratch_shapes=[
            pltpu.VMEM((rows // chunk, chunk, wide), F32),
            pltpu.VMEM((rank, wide), F32),
            pltpu.VMEM((2 * height, wide), BF16),
            pltpu.SemaphoreType.DMA((rows // chunk + 1,)),
        ],
        compiler_params=params(),
        cost_estimate=cost(12 * rows * wide * rank, 8 * rows * wide),
        name="gram_first",
    )(in_hbm(x), in_hbm(v))


def gram_again_kernel(rank, xh_ref, xl_ref, w_ref, out_ref, vcat):
    rows, wide = xh_ref.shape
    chunk = chunk_of(rows)
    vcat[...] = stacked(unpack(w_ref, rank, wide), vcat.shape[0] // 2)
    total = None
    for i in range(rows // chunk):
        part = slice(i * chunk, (i + 1) * chunk)
        term = gram_chunk(xh_ref[part, :], xl_ref[part, :], vcat)
        total = term if total is None else total + term
    pack(total[:rank, :], out_ref)


def gram_again(xh, xl, w, rank, rows_out):
    rows, wide = xh.shape
    return call(
        functools.partial(gram_again_kernel, rank),
        jax.ShapeDtypeStruct((rows_out, LANES), F32),
        (in_vmem(xh), in_vmem(xl), w),
        12 * rows * wide * rank,
        [pltpu.VMEM((2 * ceil_to(rank, LANES), wide), BF16)],
        name="gram_again",
    )


def project_kernel(
    rank, cols, groups, core_ref, me_ref, xh_ref, xl_ref, own_ref, other_ref, m_ref, w_ref, *rest
):
    out_refs = rest[:groups]
    vcat, u, whole = rest[groups:]
    rows, wide = xh_ref.shape
    chunk = chunk_of(rows)
    height = vcat.shape[0] // 2
    merge(whole, core_ref, own_ref[...], other_ref[...])
    w = dot(m_ref[...], unpack(whole, rank, wide), precision=HIGH)
    w_ref[...] = w
    vcat[...] = stacked(w, height)
    for i in range(rows // chunk):
        part = slice(i * chunk, (i + 1) * chunk)
        both = dot(xh_ref[part, :], vcat[...], NT)
        u[part, :] = both[:, :height] + both[:, height:] + dot(xl_ref[part, :], vcat[:height, :], NT)
    depth = rows // cols
    per = cols // groups
    for r in range(groups):
        first = peer(me_ref[0], r, groups) * per
        pieces = [u[pl.ds(first + k, depth, stride=cols), :][:, :rank] for k in range(per)]
        pack_block(jnp.concatenate(pieces, axis=1), out_refs[r])


def block_rows(depth, wide):
    whole, rest = divmod(wide, LANES)
    return whole * depth + (ceil_to(-(-depth // (LANES // rest)), 8) if rest else 0)


def pack_block(value, out):
    depth, wide = value.shape
    whole, rest = divmod(wide, LANES)
    for t in range(whole):
        out[t * depth : (t + 1) * depth, :] = value[:, t * LANES : (t + 1) * LANES]
    if rest:
        fold = LANES // rest
        height = ceil_to(-(-depth // fold), 8)
        tail = value[:, whole * LANES :]
        parts = []
        for q in range(fold):
            part = tail[q * height : min((q + 1) * height, depth), :]
            if part.shape[0] < height:
                part = jnp.concatenate([part, jnp.zeros((height - part.shape[0], rest), F32)], axis=0)
            parts.append(part)
        out[whole * depth :, :] = jnp.concatenate(parts, axis=1)


def unpack_block(ref, depth, wide):
    whole, rest = divmod(wide, LANES)
    parts = [ref[t * depth : (t + 1) * depth, :] for t in range(whole)]
    if rest:
        fold = LANES // rest
        height = ceil_to(-(-depth // fold), 8)
        tail = ref[whole * depth :, :]
        folded = [
            tail[: min(height, depth - q * height), q * rest : (q + 1) * rest] for q in range(fold)
        ]
        parts.append(jnp.concatenate(folded, axis=0))
    return jnp.concatenate(parts, axis=1)


def fetch_kernel(from_ref, to_ref, sem):
    copy = pltpu.make_async_copy(from_ref, to_ref, sem)
    copy.start()
    copy.wait()


def fetch(array):
    return call(
        fetch_kernel,
        pltpu.VMEM(array.shape, array.dtype),
        (in_hbm(array),),
        1e7,
        [pltpu.SemaphoreType.DMA],
        name="fetch",
        hbm=(0,),
    )


def peer(me, step, groups):
    return me ^ step if groups & (groups - 1) == 0 else lax.rem(me + step, groups)


def source(me, step, groups):
    return me ^ step if groups & (groups - 1) == 0 else lax.rem(me + groups - step, groups)


def pairs(step, groups):
    power = groups & (groups - 1) == 0
    return [(g, g ^ step if power else (g + step) % groups) for g in range(groups)]


def project(core, me, xh, xl, own, other, m, rank, cols, groups):
    rows, wide = xh.shape
    height = ceil_to(rank, LANES)
    out_rows = block_rows(rows // cols, (cols // groups) * rank)
    w, *blocks = call(
        functools.partial(project_kernel, rank, cols, groups),
        (jax.ShapeDtypeStruct((rank, wide), F32),)
        + (jax.ShapeDtypeStruct((out_rows, LANES), F32),) * groups,
        (core, me, in_vmem(xh), in_vmem(xl), own, other, m),
        6 * rows * wide * rank,
        [
            pltpu.VMEM((2 * height, wide), BF16),
            pltpu.VMEM((rows, height), F32),
            pltpu.VMEM((CORES * own.shape[0], LANES), F32),
        ],
        name="project",
        smem=(0, 1),
    )
    return w, blocks


def inverse_factor(cross, aug):
    rank = cross.shape[0]
    height, width = aug.shape[0], aug.shape[1] // 2
    row = lax.broadcasted_iota(jnp.int32, (height, width), 0)
    lane = lax.broadcasted_iota(jnp.int32, (height, width), 1)
    eye = (row == lane).astype(F32)
    aug[:, width:] = eye
    aug[:, :width] = eye
    aug[:rank, :rank] = cross
    sub = lax.broadcasted_iota(jnp.int32, (PANEL, 1), 0)
    lanes = lax.broadcasted_iota(jnp.int32, (PANEL, width), 1)

    def panel(index, carry):
        first = pl.multiple_of(index * PANEL, PANEL)
        block = aug[pl.ds(first, PANEL), :]
        left = block[:, :width]
        columns = [
            jnp.sum(jnp.where(lanes == first + c, left, 0.0), axis=1, keepdims=True)
            for c in range(PANEL)
        ]
        pivots = jnp.ones((PANEL, 1), F32)
        for r in range(PANEL):
            pivot = columns[r][r : r + 1, :]
            factor = jnp.where(sub > r, columns[r] * (1.0 / pivot), 0.0)
            pivots = jnp.where(sub == r, pivot, pivots)
            block = block - factor * block[r : r + 1, :]
            for c in range(r + 1, PANEL):
                columns[c] = columns[c] - factor * columns[c][r : r + 1, :]
        block = block / jnp.sqrt(pivots)
        aug[pl.ds(first, PANEL), :] = block
        below = jnp.where(lanes >= first + PANEL, block[:, :width], 0.0)
        aug[...] -= stacked_product(below, block)[:height]
        return carry

    lax.fori_loop(0, -(-rank // PANEL), panel, 0)
    return aug[:rank, width : width + rank]


def stacked_product(a, b):
    ah, am, al = thirds(a)
    bh, bm, bl = thirds(b)
    return dot(
        jnp.concatenate([ah, ah, am, ah, al, am], axis=0),
        jnp.concatenate([bh, bm, bh, bl, bh, bm], axis=0),
        TN,
    )


def aug_scratch(rank):
    width = ceil_to(rank, LANES)
    return pltpu.VMEM((width, 2 * width), F32)


def factor_packed_kernel(rank, wide, w_ref, m_ref, aug):
    w = unpack(w_ref, rank, wide)
    m_ref[...] = inverse_factor(dot(w, w, NT, precision=HIGH), aug)


def factor_packed(w, rank, wide):
    return call(
        functools.partial(factor_packed_kernel, rank, wide),
        jax.ShapeDtypeStruct((rank, rank), F32),
        (w,),
        3e9,
        [aug_scratch(rank)],
        name="factor_packed",
    )


def factor_basis_kernel(rank, w_ref, m_ref, basis_ref, aug):
    w = w_ref[...]
    m = inverse_factor(dot(w, w, NT, precision=HIGH), aug)
    m_ref[...] = m
    basis_ref[...] = dot(m, w, precision=HIGH)


def factor_basis(w):
    rank, wide = w.shape
    return call(
        functools.partial(factor_basis_kernel, rank),
        (jax.ShapeDtypeStruct((rank, rank), F32), jax.ShapeDtypeStruct((rank, wide), F32)),
        (w,),
        3e9,
        [aug_scratch(rank)],
        name="factor_basis",
    )


def six_products(a, b, dims):
    height = ceil_to(a.shape[0], 16)
    pad = jnp.zeros((height - a.shape[0], a.shape[1]), BF16)
    parts = thirds(a)
    if pad.shape[0]:
        parts = [jnp.concatenate([part, pad], axis=0) for part in parts]
    three = jnp.concatenate(parts, axis=0)
    first = dot(three, b[0], dims)
    second = dot(three[: 2 * height], b[1], dims)
    third = dot(three[:height], b[2], dims)
    total = (third + first[2 * height :] + second[height:]) + (first[height : 2 * height] + second[:height])
    return (total + first[:height])[: a.shape[0]]


def second_product(v, y):
    return six_products(six_products(v, y, NN), y, NT)


def second_first_kernel(per, depth, groups, core_ref, me_ref, m_ref, start_ref, *rest):
    own_refs, other_refs = rest[:groups], rest[groups : 2 * groups]
    *y_refs, out_ref, buf = rest[2 * groups :]
    rank = m_ref.shape[0]
    half = start_ref.shape[0] // CORES
    lanes = buf.shape[1] // (CORES * per)
    pad = jnp.zeros((depth, lanes - rank), F32)
    for c, u_refs in enumerate((own_refs, other_refs)):
        for r in range(groups):
            block = unpack_block(u_refs[r], depth, per * rank)
            first = pl.multiple_of(source(me_ref[0], r, groups) * depth, 8)
            for k in range(per):
                u = block[:, k * rank : (k + 1) * rank]
                u = jnp.concatenate([u, pad], axis=1) if lanes > rank else u
                place = (c * per + k) * lanes
                buf[pl.ds(first, depth), place : place + lanes] = u
    m = m_ref[...]
    if lanes > rank:
        m = jnp.concatenate([m, jnp.zeros((rank, lanes - rank), F32)], axis=1)
        m = jnp.concatenate([m, jnp.zeros((lanes - rank, lanes), F32)], axis=0)
    mt = stacked(m, lanes)
    uh, ul = split(buf[...])
    for k in range(CORES * per):
        part = slice(k * lanes, (k + 1) * lanes)
        both = dot(uh[:, part], mt, NT)
        y = both[:, :lanes] + (both[:, lanes:] + dot(ul[:, part], mt[:lanes, :], NT))
        for y_ref, third in zip(y_refs, thirds(y)):
            y_ref[:, part] = third
    start = start_ref[pl.ds(pl.multiple_of(core_ref[0] * half, half), half), :]
    pack(second_product(start, [y_ref[...] for y_ref in y_refs]), out_ref)


def second_first(core, me, own, other, m, start, per, rows_out):
    groups = len(own)
    rank2, wide = start.shape
    columns = CORES * per * ceil_to(m.shape[0], LANES)
    part = jax.ShapeDtypeStruct((wide, columns), BF16)
    *y, out = call(
        functools.partial(second_first_kernel, per, wide // groups, groups),
        (part, part, part, jax.ShapeDtypeStruct((rows_out, LANES), F32)),
        (core, me, m, start, *own, *other),
        1e8,
        [pltpu.VMEM((wide, columns), F32)],
        name="second_first",
        smem=(0, 1),
    )
    return y, out


def second_again_kernel(half, yh_ref, ym_ref, yl_ref, w_ref, out_ref):
    w = unpack(w_ref, half, yh_ref.shape[0])
    pack(second_product(w, [yh_ref[...], ym_ref[...], yl_ref[...]]), out_ref)


def second_again(y, w, half, rows_out):
    return call(
        functools.partial(second_again_kernel, half),
        jax.ShapeDtypeStruct((rows_out, LANES), F32),
        (*y, w),
        1e8,
        name="second_again",
    )


def factor_halves_kernel(half, core_ref, own_ref, other_ref, m_ref, whole, aug):
    wide = whole.shape[1]
    merge(whole, core_ref, unpack(own_ref, half, wide), unpack(other_ref, half, wide))
    w = whole[...]
    m_ref[...] = inverse_factor(dot(w, w, NT, precision=HIGH), aug)


def factor_halves(core, own, other, half, wide):
    rank2 = CORES * half
    return call(
        functools.partial(factor_halves_kernel, half),
        jax.ShapeDtypeStruct((rank2, rank2), F32),
        (core, own, other),
        3e9,
        [pltpu.VMEM((rank2, wide), F32), aug_scratch(rank2)],
        name="factor_halves",
        smem=(0,),
    )


def widen_kernel(rank, per, core_ref, own_ref, other_ref, m_ref, yh_ref, ym_ref, yl_ref, w_ref, out_ref, whole):
    rank2, wide = whole.shape
    half = rank2 // CORES
    merge(whole, core_ref, unpack(own_ref, half, wide), unpack(other_ref, half, wide))
    w = dot(m_ref[...], whole[...], precision=HIGH)
    w_ref[...] = w
    lanes = yh_ref.shape[1] // (CORES * per)
    y = [ref[:, : per * lanes] for ref in (yh_ref, ym_ref, yl_ref)]
    block = six_products(w, y, NN)
    pack_block(jnp.concatenate([block[:, k * lanes : k * lanes + rank] for k in range(per)], axis=1), out_ref)


def widen(core, own, other, m, y, per, rank):
    rank2 = m.shape[0]
    wide = y[0].shape[0]
    return call(
        functools.partial(widen_kernel, rank, per),
        (
            jax.ShapeDtypeStruct((rank2, wide), F32),
            jax.ShapeDtypeStruct((block_rows(rank2, per * rank), LANES), F32),
        ),
        (core, own, other, m, *y),
        1e8,
        [pltpu.VMEM((rank2, wide), F32)],
        name="widen",
        smem=(0,),
    )


def core_kernel(rank, per, groups, me_ref, m_ref, *rest):
    block_refs, (out_ref,) = rest[:groups], rest[groups:]
    share = out_ref.shape[0]
    rank2 = m_ref.shape[1]
    mine = m_ref[pl.ds(pl.multiple_of(me_ref[0] * share, 8), share), :]
    for r in range(groups):
        block = dot(mine, unpack_block(block_refs[r], rank2, per * rank), precision=HIGH)
        first = source(me_ref[0], r, groups) * per
        for k in range(per):
            out_ref[:, pl.ds(first + k, 1), :] = block[:, k * rank : (k + 1) * rank].reshape(share, 1, rank)


def core_blocks(me, m, blocks, per, rank):
    groups = len(blocks)
    return call(
        functools.partial(core_kernel, rank, per, groups),
        jax.ShapeDtypeStruct((m.shape[0] // groups, groups * per, rank), F32),
        (me, m, *blocks),
        1e8,
        name="core_blocks",
        smem=(0,),
    )


def sum_kernel(in_ref, out_ref):
    total = in_ref[0]
    for d in range(1, in_ref.shape[0]):
        total = total + in_ref[d]
    for d in range(out_ref.shape[0]):
        out_ref[d] = total


def total_over(value, axes, devices, alike, partners):
    rows = value.shape[0]
    share = rows // devices
    shares = lax.all_to_all(
        value.reshape(devices, share, LANES), axes, split_axis=0, concat_axis=0, tiled=True
    )
    copies = call(
        sum_kernel,
        jax.ShapeDtypeStruct((partners, share, LANES), F32),
        (shares,),
        1e6,
        name="share_sum",
    )
    whole = lax.all_to_all(copies, alike, split_axis=0, concat_axis=0, tiled=True)
    return whole.reshape(partners * share, LANES)


def local(groups, chips, tensor, start_one, start_two):
    every, alike = ("grp", "chip", "core"), ("grp", "chip")
    by_core = ("core", "grp", "chip")
    devices, partners = groups * chips * CORES, groups * chips
    depth, cols, wide = tensor.shape
    rank, rank2 = start_one.shape[1], start_two.shape[1]
    wide2 = start_two.shape[0]
    x = tensor.reshape(depth * cols, wide)
    half = rank2 // CORES
    rows = packed_rows(rank, wide, devices)
    rows2 = packed_rows(half, wide2, partners)
    per = cols // groups
    core, me = lax.axis_index("core").reshape(1), lax.axis_index("grp").reshape(1)

    def swap(value):
        return lax.ppermute(value, "core", [(i, CORES - 1 - i) for i in range(CORES)])

    p1, xh, xl = gram_first(x, start_one.T, rows)
    w1 = total_over(p1, every, devices, every, devices)
    m1 = factor_packed(w1, rank, wide)
    p2 = gram_again(xh, xl, w1, rank, rows)
    q2, m1 = lax.optimization_barrier((total_over(p2, by_core, devices, alike, partners), m1))
    q2, xl = lax.optimization_barrier((q2, xl))
    w2, u = project(core, me, xh, fetch(xl), q2, swap(q2), m1, rank, cols, groups)
    m2, basis_one = factor_basis(w2)
    own, other = [u[0]], [swap(u[0])]
    for r in range(1, groups):
        block, m2 = lax.optimization_barrier((lax.ppermute(u[r], "grp", pairs(r, groups)), m2))
        own.append(block)
        other.append(swap(block))
    y, p3 = second_first(core, me, own, other, m2, start_two.T, per, rows2)
    w3 = total_over(p3, alike, partners, alike, partners)
    p4, w3_other = lax.optimization_barrier((second_again(y, w3, half, rows2), swap(w3)))
    m3 = factor_halves(core, w3, w3_other, half, wide2)
    q4, m3 = lax.optimization_barrier((total_over(p4, alike, partners, alike, partners), m3))
    w4, mixed = widen(core, q4, swap(q4), m3, y, per, rank)
    m4, basis_two = factor_basis(w4)
    blocks = [mixed]
    for r in range(1, groups):
        block, m4 = lax.optimization_barrier((lax.ppermute(mixed, "grp", pairs(r, groups)), m4))
        blocks.append(block)
    out = core_blocks(me, m4, blocks, per, rank)
    return (basis_one.T, basis_two.T, out)


def solution(mesh):
    groups, slabs = mesh.shape["grp"], mesh.shape["slab"]
    chips = slabs // CORES
    fine = Mesh(mesh.devices.reshape(groups, chips, CORES), ("grp", "chip", "core"))
    split_spec = P("grp", ("chip", "core"), None)
    return jax.shard_map(
        functools.partial(local, groups, chips),
        mesh=fine,
        in_specs=(split_spec, P(), P()),
        out_specs=(P(), P(), split_spec),
        check_vma=False,
    )
```

```python
import functools

import jax
import jax.numpy as jnp
from jax import lax
from jax.experimental import pallas as pl
from jax.experimental.pallas import tpu as pltpu
from jax.sharding import Mesh
from jax.sharding import PartitionSpec as P

HIGH = lax.Precision.HIGHEST
F32, BF16 = jnp.float32, jnp.bfloat16
LANES = 128
PANEL = 16
CORES = 2
NN = (((1,), (0,)), ((), ()))
NT = (((1,), (1,)), ((), ()))
TN = (((0,), (0,)), ((), ()))


def dot(a, b, dims=NN, precision=None):
    return lax.dot_general(a, b, dims, precision=precision, preferred_element_type=F32)


def split(value):
    high = value.astype(BF16)
    low = (value - high.astype(F32)).astype(BF16)
    return high, low


def thirds(value):
    high = value.astype(BF16)
    rest = value - high.astype(F32)
    middle = rest.astype(BF16)
    return high, middle, (rest - middle.astype(F32)).astype(BF16)


def stacked(value, height):
    high, low = split(value)
    pad = jnp.zeros((height - value.shape[0], value.shape[1]), BF16)
    if pad.shape[0]:
        high, low = (jnp.concatenate([half, pad], axis=0) for half in (high, low))
    return jnp.concatenate([high, low], axis=0)


def ceil_to(value, unit):
    return -(-value // unit) * unit


def packed_rows(rank, wide, devices):
    dense = -(-rank * wide // LANES)
    return devices * ceil_to(-(-dense // devices), 8)


def pack(value, out):
    rank, wide = value.shape
    whole, rest = divmod(wide, LANES)
    for t in range(whole):
        out[t * rank : (t + 1) * rank, :] = value[:, t * LANES : (t + 1) * LANES]
    row = whole * rank
    if rest:
        groups = LANES // rest
        height = rank // groups
        tail = value[:, whole * LANES :]
        out[row : row + height, :] = jnp.concatenate(
            [tail[q * height : (q + 1) * height, :] for q in range(groups)], axis=1
        )
        row += height
    if row < out.shape[0]:
        out[row:, :] = jnp.zeros((out.shape[0] - row, LANES), F32)


def unpack(ref, rank, wide):
    whole, rest = divmod(wide, LANES)
    parts = [ref[t * rank : (t + 1) * rank, :] for t in range(whole)]
    if rest:
        groups = LANES // rest
        height = rank // groups
        tail = ref[whole * rank : whole * rank + height, :]
        parts.append(
            jnp.concatenate([tail[:, q * rest : (q + 1) * rest] for q in range(groups)], axis=0)
        )
    return jnp.concatenate(parts, axis=1)


def merge(whole, core_ref, own, other):
    half = own.shape[0]
    core = core_ref[0]
    whole[pl.ds(pl.multiple_of(core * half, half), half), :] = own
    whole[pl.ds(pl.multiple_of((1 - core) * half, half), half), :] = other


def merge_shares(whole, core_ref, own_ref, other_ref):
    partners, share, _ = own_ref.shape
    core = core_ref[0]
    for p in range(partners):
        first = pl.multiple_of((p * CORES + core) * share, share)
        whole[pl.ds(first, share), :] = own_ref[p]
        first = pl.multiple_of((p * CORES + 1 - core) * share, share)
        whole[pl.ds(first, share), :] = other_ref[p]


def cost(flops, moved):
    return pl.CostEstimate(flops=int(flops), bytes_accessed=int(moved), transcendentals=0)


def in_hbm(array):
    return pltpu.with_memory_space_constraint(array, pltpu.HBM)


def in_vmem(array):
    return pltpu.with_memory_space_constraint(array, pltpu.VMEM)


def params():
    return pltpu.CompilerParams(vmem_limit_bytes=20 * 1024 * 1024)


def call(kernel, outs, args, flops, scratch=(), name=None, hbm=(), smem=()):
    return pl.pallas_call(
        kernel,
        out_shape=outs,
        in_specs=[
            pl.BlockSpec(
                memory_space=pltpu.HBM if i in hbm else pltpu.SMEM if i in smem else pltpu.VMEM
            )
            for i in range(len(args))
        ],
        out_specs=jax.tree.map(lambda _: pl.BlockSpec(memory_space=pltpu.VMEM), outs),
        scratch_shapes=list(scratch),
        compiler_params=params(),
        cost_estimate=cost(flops, sum(a.size * 4 for a in args)),
        name=name,
    )(*args)


def chunk_of(rows):
    return max(c for c in range(16, 513, 16) if rows % c == 0)


def gram_chunk(xh, xl, vcat):
    height = vcat.shape[0] // 2
    both = dot(vcat[...], xh, NT)
    z = both[:height] + both[height:] + dot(vcat[:height, :], xl, NT)
    zcat = stacked(z, height)
    both = dot(zcat, xh)
    return both[:height] + both[height:] + dot(zcat[:height, :], xl)


def gram_first_kernel(x_hbm, v_hbm, out_ref, xh_ref, xl_hbm, xbuf, lbuf, vbuf, vcat, sems, low_sems):
    steps, chunk, _ = xbuf.shape
    writes = [
        pltpu.make_async_copy(lbuf.at[i], xl_hbm.at[pl.ds(i * chunk, chunk), :], low_sems.at[i])
        for i in range(steps)
    ]
    start = pltpu.make_async_copy(v_hbm, vbuf, sems.at[steps])
    start.start()
    copies = [
        pltpu.make_async_copy(x_hbm.at[pl.ds(i * chunk, chunk), :], xbuf.at[i], sems.at[i])
        for i in range(steps)
    ]
    for copy in copies:
        copy.start()
    start.wait()
    vcat[...] = stacked(vbuf[...], vcat.shape[0] // 2)
    total = None
    for i in range(steps):
        copies[i].wait()
        xh, xl = split(xbuf[i])
        xh_ref[i * chunk : (i + 1) * chunk, :] = xh
        lbuf[i] = xl
        writes[i].start()
        term = gram_chunk(xh, xl, vcat)
        total = term if total is None else total + term
    pack(total[: vbuf.shape[0], :], out_ref)
    for write in writes:
        write.wait()


def gram_first(x, v, rows_out):
    rows, wide = x.shape
    rank = v.shape[0]
    chunk = chunk_of(rows)
    height = ceil_to(rank, LANES)
    vmem = pl.BlockSpec(memory_space=pltpu.VMEM)
    hbm = pl.BlockSpec(memory_space=pltpu.HBM)
    return pl.pallas_call(
        gram_first_kernel,
        out_shape=(
            jax.ShapeDtypeStruct((rows_out, LANES), F32),
            pltpu.VMEM((rows, wide), BF16),
            pltpu.HBM((rows, wide), BF16),
        ),
        in_specs=[hbm, hbm],
        out_specs=(vmem, vmem, pl.BlockSpec(memory_space=pltpu.HBM)),
        scratch_shapes=[
            pltpu.VMEM((rows // chunk, chunk, wide), F32),
            pltpu.VMEM((rows // chunk, chunk, wide), BF16),
            pltpu.VMEM((rank, wide), F32),
            pltpu.VMEM((2 * height, wide), BF16),
            pltpu.SemaphoreType.DMA((rows // chunk + 1,)),
            pltpu.SemaphoreType.DMA((rows // chunk,)),
        ],
        compiler_params=params(),
        cost_estimate=cost(12 * rows * wide * rank, 8 * rows * wide),
        name="gram_first",
    )(in_hbm(x), in_hbm(v))


def gram_again_kernel(rank, core_ref, xh_ref, xl_ref, own_ref, other_ref, out_ref, vcat, whole):
    rows, wide = xh_ref.shape
    chunk = chunk_of(rows)
    merge_shares(whole, core_ref, own_ref, other_ref)
    vcat[...] = stacked(unpack(whole, rank, wide), vcat.shape[0] // 2)
    total = None
    for i in range(rows // chunk):
        part = slice(i * chunk, (i + 1) * chunk)
        term = gram_chunk(xh_ref[part, :], xl_ref[part, :], vcat)
        total = term if total is None else total + term
    pack(total[:rank, :], out_ref)


def gram_again(core, xh, xl, own, other, rank, rows_out):
    rows, wide = xh.shape
    return call(
        functools.partial(gram_again_kernel, rank),
        jax.ShapeDtypeStruct((rows_out, LANES), F32),
        (core, in_vmem(xh), in_vmem(xl), own, other),
        12 * rows * wide * rank,
        [pltpu.VMEM((2 * ceil_to(rank, LANES), wide), BF16), pltpu.VMEM((rows_out, LANES), F32)],
        name="gram_again",
        smem=(0,),
    )


def project_kernel(
    rank, cols, groups, core_ref, me_ref, xh_ref, xl_ref, own_ref, other_ref, m_ref, w_ref, *rest
):
    out_refs = rest[:groups]
    vcat, u, whole = rest[groups:]
    rows, wide = xh_ref.shape
    chunk = chunk_of(rows)
    height = vcat.shape[0] // 2
    merge_shares(whole, core_ref, own_ref, other_ref)
    w = dot(m_ref[...], unpack(whole, rank, wide), precision=HIGH)
    w_ref[...] = w
    vcat[...] = stacked(w, height)
    for i in range(rows // chunk):
        part = slice(i * chunk, (i + 1) * chunk)
        both = dot(xh_ref[part, :], vcat[...], NT)
        u[part, :] = both[:, :height] + both[:, height:] + dot(xl_ref[part, :], vcat[:height, :], NT)
    depth = rows // cols
    per = cols // groups
    for r in range(groups):
        first = peer(me_ref[0], r, groups) * per
        pieces = [u[pl.ds(first + k, depth, stride=cols), :][:, :rank] for k in range(per)]
        pack_block(jnp.concatenate(pieces, axis=1), out_refs[r])


def block_rows(depth, wide):
    whole, rest = divmod(wide, LANES)
    return whole * depth + (ceil_to(-(-depth // (LANES // rest)), 8) if rest else 0)


def pack_block(value, out):
    depth, wide = value.shape
    whole, rest = divmod(wide, LANES)
    for t in range(whole):
        out[t * depth : (t + 1) * depth, :] = value[:, t * LANES : (t + 1) * LANES]
    if rest:
        fold = LANES // rest
        height = ceil_to(-(-depth // fold), 8)
        tail = value[:, whole * LANES :]
        parts = []
        for q in range(fold):
            part = tail[q * height : min((q + 1) * height, depth), :]
            if part.shape[0] < height:
                part = jnp.concatenate([part, jnp.zeros((height - part.shape[0], rest), F32)], axis=0)
            parts.append(part)
        out[whole * depth :, :] = jnp.concatenate(parts, axis=1)


def unpack_block(ref, depth, wide):
    whole, rest = divmod(wide, LANES)
    parts = [ref[t * depth : (t + 1) * depth, :] for t in range(whole)]
    if rest:
        fold = LANES // rest
        height = ceil_to(-(-depth // fold), 8)
        tail = ref[whole * depth :, :]
        folded = [
            tail[: min(height, depth - q * height), q * rest : (q + 1) * rest] for q in range(fold)
        ]
        parts.append(jnp.concatenate(folded, axis=0))
    return jnp.concatenate(parts, axis=1)


def fetch_kernel(from_ref, to_ref, sem):
    copy = pltpu.make_async_copy(from_ref, to_ref, sem)
    copy.start()
    copy.wait()


def fetch(array):
    return call(
        fetch_kernel,
        pltpu.VMEM(array.shape, array.dtype),
        (in_hbm(array),),
        1e7,
        [pltpu.SemaphoreType.DMA],
        name="fetch",
        hbm=(0,),
    )


def peer(me, step, groups):
    return me ^ step if groups & (groups - 1) == 0 else lax.rem(me + step, groups)


def source(me, step, groups):
    return me ^ step if groups & (groups - 1) == 0 else lax.rem(me + groups - step, groups)


def pairs(step, groups):
    power = groups & (groups - 1) == 0
    return [(g, g ^ step if power else (g + step) % groups) for g in range(groups)]


def project(core, me, xh, xl, own, other, m, rank, cols, groups):
    rows, wide = xh.shape
    height = ceil_to(rank, LANES)
    out_rows = block_rows(rows // cols, (cols // groups) * rank)
    w, *blocks = call(
        functools.partial(project_kernel, rank, cols, groups),
        (jax.ShapeDtypeStruct((rank, wide), F32),)
        + (jax.ShapeDtypeStruct((out_rows, LANES), F32),) * groups,
        (core, me, in_vmem(xh), in_vmem(xl), own, other, m),
        6 * rows * wide * rank,
        [
            pltpu.VMEM((2 * height, wide), BF16),
            pltpu.VMEM((rows, height), F32),
            pltpu.VMEM((CORES * own.shape[0] * own.shape[1], LANES), F32),
        ],
        name="project",
        smem=(0, 1),
    )
    return w, blocks


def inverse_factor(cross, aug):
    rank = cross.shape[0]
    height, width = aug.shape[0], aug.shape[1] // 2
    row = lax.broadcasted_iota(jnp.int32, (height, width), 0)
    lane = lax.broadcasted_iota(jnp.int32, (height, width), 1)
    eye = (row == lane).astype(F32)
    aug[:, width:] = eye
    aug[:, :width] = eye
    aug[:rank, :rank] = cross
    sub = lax.broadcasted_iota(jnp.int32, (PANEL, 1), 0)
    lanes = lax.broadcasted_iota(jnp.int32, (PANEL, width), 1)

    def panel(index, carry):
        first = pl.multiple_of(index * PANEL, PANEL)
        block = aug[pl.ds(first, PANEL), :]
        left = block[:, :width]
        columns = [
            jnp.sum(jnp.where(lanes == first + c, left, 0.0), axis=1, keepdims=True)
            for c in range(PANEL)
        ]
        pivots = jnp.ones((PANEL, 1), F32)
        for r in range(PANEL):
            pivot = columns[r][r : r + 1, :]
            factor = jnp.where(sub > r, columns[r] * (1.0 / pivot), 0.0)
            pivots = jnp.where(sub == r, pivot, pivots)
            block = block - factor * block[r : r + 1, :]
            for c in range(r + 1, PANEL):
                columns[c] = columns[c] - factor * columns[c][r : r + 1, :]
        block = block / jnp.sqrt(pivots)
        aug[pl.ds(first, PANEL), :] = block
        below = jnp.where(lanes >= first + PANEL, block[:, :width], 0.0)
        aug[...] -= stacked_product(below, block)[:height]
        return carry

    lax.fori_loop(0, -(-rank // PANEL), panel, 0)
    return aug[:rank, width : width + rank]


def stacked_product(a, b):
    ah, am, al = thirds(a)
    bh, bm, bl = thirds(b)
    return dot(
        jnp.concatenate([ah, ah, am, ah, al, am], axis=0),
        jnp.concatenate([bh, bm, bh, bl, bh, bm], axis=0),
        TN,
    )


def aug_scratch(rank):
    width = ceil_to(rank, LANES)
    return pltpu.VMEM((width, 2 * width), F32)


def factor_packed_kernel(rank, wide, core_ref, own_ref, other_ref, m_ref, whole, aug):
    merge_shares(whole, core_ref, own_ref, other_ref)
    w = unpack(whole, rank, wide)
    m_ref[...] = inverse_factor(dot(w, w, NT, precision=HIGH), aug)


def factor_packed(core, own, other, rank, wide):
    return call(
        functools.partial(factor_packed_kernel, rank, wide),
        jax.ShapeDtypeStruct((rank, rank), F32),
        (core, own, other),
        3e9,
        [pltpu.VMEM((CORES * own.shape[0] * own.shape[1], LANES), F32), aug_scratch(rank)],
        name="factor_packed",
        smem=(0,),
    )


def factor_basis_kernel(rank, w_ref, m_ref, basis_ref, aug):
    w = w_ref[...]
    m = inverse_factor(dot(w, w, NT, precision=HIGH), aug)
    m_ref[...] = m
    basis_ref[...] = dot(m, w, precision=HIGH)


def factor_basis(w):
    rank, wide = w.shape
    return call(
        functools.partial(factor_basis_kernel, rank),
        (jax.ShapeDtypeStruct((rank, rank), F32), jax.ShapeDtypeStruct((rank, wide), F32)),
        (w,),
        3e9,
        [aug_scratch(rank)],
        name="factor_basis",
    )


def six_products(a, b, dims):
    height = ceil_to(a.shape[0], 16)
    pad = jnp.zeros((height - a.shape[0], a.shape[1]), BF16)
    parts = thirds(a)
    if pad.shape[0]:
        parts = [jnp.concatenate([part, pad], axis=0) for part in parts]
    three = jnp.concatenate(parts, axis=0)
    first = dot(three, b[0], dims)
    second = dot(three[: 2 * height], b[1], dims)
    third = dot(three[:height], b[2], dims)
    total = (third + first[2 * height :] + second[height:]) + (first[height : 2 * height] + second[:height])
    return (total + first[:height])[: a.shape[0]]


def second_product(v, y):
    return six_products(six_products(v, y, NN), y, NT)


def second_first_kernel(per, depth, groups, core_ref, me_ref, m_ref, start_ref, *rest):
    own_refs, other_refs = rest[:groups], rest[groups : 2 * groups]
    *y_refs, out_ref, buf = rest[2 * groups :]
    rank = m_ref.shape[0]
    half = start_ref.shape[0] // CORES
    lanes = buf.shape[1] // (CORES * per)
    pad = jnp.zeros((depth, lanes - rank), F32)
    for c, u_refs in enumerate((own_refs, other_refs)):
        for r in range(groups):
            block = unpack_block(u_refs[r], depth, per * rank)
            first = pl.multiple_of(source(me_ref[0], r, groups) * depth, 8)
            for k in range(per):
                u = block[:, k * rank : (k + 1) * rank]
                u = jnp.concatenate([u, pad], axis=1) if lanes > rank else u
                place = (c * per + k) * lanes
                buf[pl.ds(first, depth), place : place + lanes] = u
    m = m_ref[...]
    if lanes > rank:
        m = jnp.concatenate([m, jnp.zeros((rank, lanes - rank), F32)], axis=1)
        m = jnp.concatenate([m, jnp.zeros((lanes - rank, lanes), F32)], axis=0)
    mt = stacked(m, lanes)
    uh, ul = split(buf[...])
    for k in range(CORES * per):
        part = slice(k * lanes, (k + 1) * lanes)
        both = dot(uh[:, part], mt, NT)
        y = both[:, :lanes] + (both[:, lanes:] + dot(ul[:, part], mt[:lanes, :], NT))
        for y_ref, third in zip(y_refs, thirds(y)):
            y_ref[:, part] = third
    start = start_ref[pl.ds(pl.multiple_of(core_ref[0] * half, half), half), :]
    pack(second_product(start, [y_ref[...] for y_ref in y_refs]), out_ref)


def second_first(core, me, own, other, m, start, per, rows_out):
    groups = len(own)
    rank2, wide = start.shape
    columns = CORES * per * ceil_to(m.shape[0], LANES)
    part = jax.ShapeDtypeStruct((wide, columns), BF16)
    *y, out = call(
        functools.partial(second_first_kernel, per, wide // groups, groups),
        (part, part, part, jax.ShapeDtypeStruct((rows_out, LANES), F32)),
        (core, me, m, start, *own, *other),
        1e8,
        [pltpu.VMEM((wide, columns), F32)],
        name="second_first",
        smem=(0, 1),
    )
    return y, out


def second_again_kernel(half, yh_ref, ym_ref, yl_ref, w_ref, out_ref):
    w = unpack(w_ref, half, yh_ref.shape[0])
    pack(second_product(w, [yh_ref[...], ym_ref[...], yl_ref[...]]), out_ref)


def second_again(y, w, half, rows_out):
    return call(
        functools.partial(second_again_kernel, half),
        jax.ShapeDtypeStruct((rows_out, LANES), F32),
        (*y, w),
        1e8,
        name="second_again",
    )


def factor_halves_kernel(half, core_ref, own_ref, other_ref, m_ref, whole, aug):
    wide = whole.shape[1]
    merge(whole, core_ref, unpack(own_ref, half, wide), unpack(other_ref, half, wide))
    w = whole[...]
    m_ref[...] = inverse_factor(dot(w, w, NT, precision=HIGH), aug)


def factor_halves(core, own, other, half, wide):
    rank2 = CORES * half
    return call(
        functools.partial(factor_halves_kernel, half),
        jax.ShapeDtypeStruct((rank2, rank2), F32),
        (core, own, other),
        3e9,
        [pltpu.VMEM((rank2, wide), F32), aug_scratch(rank2)],
        name="factor_halves",
        smem=(0,),
    )


def widen_kernel(rank, per, core_ref, own_ref, other_ref, m_ref, yh_ref, ym_ref, yl_ref, w_ref, out_ref, whole):
    rank2, wide = whole.shape
    half = rank2 // CORES
    merge(whole, core_ref, unpack(own_ref, half, wide), unpack(other_ref, half, wide))
    w = dot(m_ref[...], whole[...], precision=HIGH)
    w_ref[...] = w
    lanes = yh_ref.shape[1] // (CORES * per)
    y = [ref[:, : per * lanes] for ref in (yh_ref, ym_ref, yl_ref)]
    block = six_products(w, y, NN)
    pack_block(jnp.concatenate([block[:, k * lanes : k * lanes + rank] for k in range(per)], axis=1), out_ref)


def widen(core, own, other, m, y, per, rank):
    rank2 = m.shape[0]
    wide = y[0].shape[0]
    return call(
        functools.partial(widen_kernel, rank, per),
        (
            jax.ShapeDtypeStruct((rank2, wide), F32),
            jax.ShapeDtypeStruct((block_rows(rank2, per * rank), LANES), F32),
        ),
        (core, own, other, m, *y),
        1e8,
        [pltpu.VMEM((rank2, wide), F32)],
        name="widen",
        smem=(0,),
    )


def core_kernel(rank, per, groups, me_ref, m_ref, *rest):
    block_refs, (out_ref,) = rest[:groups], rest[groups:]
    share = out_ref.shape[0]
    rank2 = m_ref.shape[1]
    mine = m_ref[pl.ds(pl.multiple_of(me_ref[0] * share, 8), share), :]
    for r in range(groups):
        block = dot(mine, unpack_block(block_refs[r], rank2, per * rank), precision=HIGH)
        first = source(me_ref[0], r, groups) * per
        for k in range(per):
            out_ref[:, pl.ds(first + k, 1), :] = block[:, k * rank : (k + 1) * rank].reshape(share, 1, rank)


def core_blocks(me, m, blocks, per, rank):
    groups = len(blocks)
    return call(
        functools.partial(core_kernel, rank, per, groups),
        jax.ShapeDtypeStruct((m.shape[0] // groups, groups * per, rank), F32),
        (me, m, *blocks),
        1e8,
        name="core_blocks",
        smem=(0,),
    )


def sum_kernel(in_ref, out_ref):
    total = in_ref[0]
    for d in range(1, in_ref.shape[0]):
        total = total + in_ref[d]
    for d in range(out_ref.shape[0]):
        out_ref[d] = total


def total_over(value, axes, devices, alike, partners):
    rows = value.shape[0]
    share = rows // devices
    shares = lax.all_to_all(
        value.reshape(devices, share, LANES), axes, split_axis=0, concat_axis=0, tiled=True
    )
    copies = call(
        sum_kernel,
        jax.ShapeDtypeStruct((partners, share, LANES), F32),
        (shares,),
        1e6,
        name="share_sum",
    )
    whole = lax.all_to_all(copies, alike, split_axis=0, concat_axis=0, tiled=True)
    return whole.reshape(partners * share, LANES)


def local(groups, chips, tensor, start_one, start_two):
    every, alike = ("grp", "chip", "core"), ("grp", "chip")
    devices, partners = groups * chips * CORES, groups * chips
    depth, cols, wide = tensor.shape
    rank, rank2 = start_one.shape[1], start_two.shape[1]
    wide2 = start_two.shape[0]
    x = tensor.reshape(depth * cols, wide)
    half = rank2 // CORES
    rows = packed_rows(rank, wide, devices)
    rows2 = packed_rows(half, wide2, partners)
    per = cols // groups
    core, me = lax.axis_index("core").reshape(1), lax.axis_index("grp").reshape(1)

    def swap(value):
        return lax.ppermute(value, "core", [(i, CORES - 1 - i) for i in range(CORES)])

    p1, xh, xl = gram_first(x, start_one.T, rows)
    w1 = total_over(p1, every, devices, alike, partners).reshape(partners, -1, LANES)
    w1, xl = lax.optimization_barrier((w1, xl))
    w1_other = swap(w1)
    m1 = factor_packed(core, w1, w1_other, rank, wide)
    p2 = gram_again(core, xh, fetch(xl), w1, w1_other, rank, rows)
    q2, m1 = lax.optimization_barrier((total_over(p2, every, devices, alike, partners), m1))
    q2, xl = lax.optimization_barrier((q2.reshape(partners, -1, LANES), xl))
    w2, u = project(core, me, xh, fetch(xl), q2, swap(q2), m1, rank, cols, groups)
    m2, basis_one = factor_basis(w2)
    own, other = [u[0]], [swap(u[0])]
    for r in range(1, groups):
        block, m2 = lax.optimization_barrier((lax.ppermute(u[r], "grp", pairs(r, groups)), m2))
        own.append(block)
        other.append(swap(block))
    y, p3 = second_first(core, me, own, other, m2, start_two.T, per, rows2)
    w3 = total_over(p3, alike, partners, alike, partners)
    p4, w3_other = lax.optimization_barrier((second_again(y, w3, half, rows2), swap(w3)))
    m3 = factor_halves(core, w3, w3_other, half, wide2)
    q4, m3 = lax.optimization_barrier((total_over(p4, alike, partners, alike, partners), m3))
    w4, mixed = widen(core, q4, swap(q4), m3, y, per, rank)
    m4, basis_two = factor_basis(w4)
    blocks = [mixed]
    for r in range(1, groups):
        block, m4 = lax.optimization_barrier((lax.ppermute(mixed, "grp", pairs(r, groups)), m4))
        blocks.append(block)
    out = core_blocks(me, m4, blocks, per, rank)
    return (basis_one.T, basis_two.T, out)


def solution(mesh):
    groups, slabs = mesh.shape["grp"], mesh.shape["slab"]
    chips = slabs // CORES
    fine = Mesh(mesh.devices.reshape(groups, chips, CORES), ("grp", "chip", "core"))
    split_spec = P("grp", ("chip", "core"), None)
    return jax.shard_map(
        functools.partial(local, groups, chips),
        mesh=fine,
        in_specs=(split_spec, P(), P()),
        out_specs=(P(), P(), split_spec),
        check_vma=False,
    )
```
